32 devices in a mesh: gx: 8 (over y, x, core), gy: 4 (over z).
Axes of the slice: x: 2, y: 2, z: 4, core: 2. Of those that a mesh axis runs over, the one named last changes fastest.
Arguments:
- nodes: bfloat16 [32768, 128], P(('gx', 'gy')), may hold values from -6 to 6
- ghost_rows: int32 [32, 8, 256], P(('gx', 'gy')), may hold values from 0 to 1023
- ghost_count: int32 [32, 8], P(('gx', 'gy')), may hold values from 0 to 256, as said below
- edge_send: int32 [32, 4096], P(('gx', 'gy')), may hold values from 0 to 3071
- edge_recv: int32 [32, 4096], P(('gx', 'gy')), may hold values from 0 to 1023
- edge_count: int32 [32], P(('gx', 'gy')), may hold values from 512 to 4096, as said below
- pool_map: int32 [32, 1024], P(('gx', 'gy')), may hold values from 0 to 191, as said below
- w_edge_in: bfloat16 [256, 128], replicated, may hold values from -0.375 to 0.375
- w_edge_out: bfloat16 [128, 128], replicated, may hold values from -0.5 to 0.5
- w_node_in: bfloat16 [256, 128], replicated, may hold values from -0.375 to 0.375
- w_node_out: bfloat16 [128, 128], replicated, may hold values from -0.5 to 0.5
- w_coarse_in: bfloat16 [128, 128], replicated, may hold values from -0.5 to 0.5
- w_coarse_out: bfloat16 [128, 128], replicated, may hold values from -0.5 to 0.5
- d_fine: bfloat16 [32768, 128], P(('gx', 'gy')), may hold values from -6 to 6
- d_coarse: bfloat16 [4096, 128], P(('gx', 'gy')), may hold values from -6 to 6
Outputs:
- fine_out: bfloat16 [32768, 128], P(('gx', 'gy'))
- coarse_out: bfloat16 [4096, 128], P(('gx', 'gy'))
- grad_nodes: float32 [32768, 128], P(('gx', 'gy'))
- grad_edge_in: float32 [256, 128], replicated
- grad_edge_out: float32 [128, 128], replicated
- grad_node_in: float32 [256, 128], replicated
- grad_node_out: float32 [128, 128], replicated
- grad_coarse_in: float32 [128, 128], replicated
- grad_coarse_out: float32 [128, 128], replicated
The draws below stay inside these ranges and needn't reach their ends.
Inputs may be any that keep to these rules, and one draw needn't show every extreme that they name: `ghost_count`: every device fills all 256 slots for at least one offset. `edge_count`: at least one device has all 4096 slots live. `pool_map`: values under 32 occur only on devices that are not first along gy, and values of 160 or more only on devices that are not last along gy, so every parent lies in the device's gx column.
All inputs are finite; a program needn't handle non-finite values.
Results may differ from the reference program's by a relative error of at most 0.012.
Values may be sent and summed in bfloat16 or wider, within the bound.
A program may use at most 64 MiB of HBM per device.

```python
import jax
import jax.numpy as jnp
from jax import lax

C = 128
HID = 128
GBLK = 256
BAND = 32
NODE_DEV = 1024
EDGE_DEV = 4096
CO_DEV = 128
NODES = 32768
COARSE = 4096
N_GX = 8
N_GY = 4
DEVICES = 32


def draw_ghost_count(key, part):
    key_one, key_two = jax.random.split(jax.random.fold_in(key, 11))
    counts = jax.random.randint(key_one, (N_GX * N_GY, 8), 0, GBLK + 1)
    full_peer = jax.random.randint(key_two, (N_GX * N_GY, 1), 0, 8)
    direction_ids = jnp.arange(8, dtype=jnp.int32)[None, :]
    return jnp.where(direction_ids == full_peer, GBLK, counts).astype(jnp.int32)


def draw_edge_count(key, part):
    key_one, key_two = jax.random.split(jax.random.fold_in(key, 23))
    shifts = jax.random.randint(key_one, (N_GX * N_GY,), 0, 4).astype(jnp.int32)
    counts = jnp.right_shift(jnp.full((N_GX * N_GY,), EDGE_DEV, jnp.int32), shifts)
    busiest = jax.random.randint(key_two, (), 0, N_GX * N_GY)
    device_ids = jnp.arange(N_GX * N_GY, dtype=jnp.int32)
    return jnp.where(device_ids == busiest, EDGE_DEV, counts).astype(jnp.int32)


def draw_pool_map(key, part):
    devices = N_GX * N_GY
    near = max(1, NODE_DEV // 16)
    key_one, key_two, key_three, key_four = jax.random.split(jax.random.fold_in(key, 37), 4)
    order = jax.vmap(lambda single: jax.random.permutation(single, NODE_DEV))(jax.random.split(key_one, devices))
    own_parent = jax.random.randint(key_two, (devices, NODE_DEV), BAND, BAND + CO_DEV)
    lower_parent = jax.random.randint(key_three, (devices, NODE_DEV), 0, BAND)
    upper_parent = jax.random.randint(key_four, (devices, NODE_DEV), BAND + CO_DEV, CO_DEV + 2 * BAND)
    row_idx = (jnp.arange(devices, dtype=jnp.int32) % N_GY)[:, None]
    goes_lower = (order < near) & (row_idx > 0)
    goes_upper = (order >= near) & (order < 2 * near) & (row_idx < N_GY - 1)
    return jnp.where(goes_lower, lower_parent, jnp.where(goes_upper, upper_parent, own_parent)).astype(jnp.int32)


def set_ends(drawn, own_key, low, top_value):
    longest = drawn.shape.index(max(drawn.shape))
    spots = []
    for shift in (0, 1):
        where = [jax.random.randint(jax.random.fold_in(own_key, axis), (), 0, length) for axis, length in enumerate(drawn.shape)]
        where[longest] = (where[longest] + shift) % drawn.shape[longest]
        spots.append(tuple(where))
    return drawn.at[spots[0]].set(low).at[spots[1]].set(top_value)


def level_of(key, dims, cuts, smallest, largest):
    def one(axis_at, blocks):
        draws = jax.random.uniform(jax.random.fold_in(jax.random.fold_in(key, 6), axis_at), (blocks,), jnp.float32, smallest / len(cuts), largest / len(cuts))
        return jnp.repeat(jnp.exp(draws), dims[axis_at] // blocks).reshape((-1,) + (1,) * (len(dims) - axis_at - 1))

    loudness = one(*cuts[0])
    for cut in cuts[1:]:
        loudness = loudness * one(*cut)
    return loudness


def normal_values(rng, dims, scale, reach, shards=(), kind=jnp.bfloat16):
    gain = level_of(rng, dims, shards, -0.22, 0.18) if shards else 1.0
    entries = jax.random.normal(rng, dims, jnp.float32) * scale * gain
    return jnp.minimum(jnp.maximum(entries, -reach), reach).astype(kind)


def setup_inputs(seed: int = 0) -> dict:
    splits = jax.random.split(jax.random.key(seed), 16)
    return {
        "nodes": normal_values(splits[0], (NODES, C), 1.0, 6.0, ((0, 32),)),
        "ghost_rows": set_ends(jax.random.randint(splits[1], (DEVICES, 8, GBLK), 0, NODE_DEV), jax.random.fold_in(splits[1], 1), 0, NODE_DEV - 1).astype(jnp.int32),
        "ghost_count": draw_ghost_count(jax.random.fold_in(splits[15], 71), 0),
        "edge_send": set_ends(jax.random.randint(splits[3], (DEVICES, EDGE_DEV), 0, NODE_DEV + 8 * GBLK), jax.random.fold_in(splits[3], 1), 0, (NODE_DEV + 8 * GBLK) - 1).astype(jnp.int32),
        "edge_recv": set_ends(jax.random.randint(splits[4], (DEVICES, EDGE_DEV), 0, NODE_DEV), jax.random.fold_in(splits[4], 1), 0, NODE_DEV - 1).astype(jnp.int32),
        "edge_count": draw_edge_count(jax.random.fold_in(splits[15], 71), 0),
        "pool_map": draw_pool_map(jax.random.fold_in(splits[15], 71), 0),
        "w_edge_in": normal_values(splits[7], (2 * C, HID), (2 * C) ** -0.5, 0.375),
        "w_edge_out": normal_values(splits[8], (HID, C), HID ** -0.5, 0.5),
        "w_node_in": normal_values(splits[9], (2 * C, HID), (2 * C) ** -0.5, 0.375),
        "w_node_out": normal_values(splits[10], (HID, C), HID ** -0.5, 0.5),
        "w_coarse_in": normal_values(splits[11], (C, HID), C ** -0.5, 0.5),
        "w_coarse_out": normal_values(splits[12], (HID, C), HID ** -0.5, 0.5),
        "d_fine": normal_values(splits[13], (NODES, C), 1.0, 6.0, ((0, 32),)),
        "d_coarse": normal_values(splits[14], (COARSE, C), 1.0, 6.0, ((0, 32),)),
    }


offset_across = (-1, -1, -1, 0, 0, 1, 1, 1)
offset_along = (-1, 0, 1, -1, 1, -1, 0, 1)


def matmul(left, right):
    return jnp.dot(left, right, preferred_element_type=jnp.float32)


def silu_slope(pre_value):
    sigmoid_v = jax.nn.sigmoid(pre_value)
    return sigmoid_v * (1.0 + pre_value * (1.0 - sigmoid_v))


def fine_forward(owned, ghosts, send_index, recv_index, edge_live, weights):
    w_edge_in, w_edge_out, w_node_in, w_node_out = weights
    latent = owned.shape[1]
    lookup = jnp.concatenate([owned, ghosts], axis=0)
    senders = lookup[send_index]
    receivers = owned[recv_index]
    edge_pre = matmul(senders, w_edge_in[:latent]) + matmul(receivers, w_edge_in[latent:])
    edge_act = jax.nn.silu(edge_pre).astype(jnp.bfloat16)
    message = (matmul(edge_act, w_edge_out) * edge_live[:, None]).astype(jnp.bfloat16)
    summed = jax.ops.segment_sum(message.astype(jnp.float32), recv_index, num_segments=owned.shape[0]).astype(jnp.bfloat16)
    node_pre = matmul(owned, w_node_in[:latent]) + matmul(summed, w_node_in[latent:])
    node_act = jax.nn.silu(node_pre).astype(jnp.bfloat16)
    fine_out = (owned.astype(jnp.float32) + matmul(node_act, w_node_out)).astype(jnp.bfloat16)
    return fine_out, (senders, receivers, edge_pre, edge_act, summed, node_pre, node_act)


def fine_backward(owned, send_index, recv_index, edge_live, weights, stashed, d_total, lookup_rows):
    w_edge_in, w_edge_out, w_node_in, w_node_out = weights
    senders, receivers, edge_pre, edge_act, summed, node_pre, node_act = stashed
    rows_here, latent = owned.shape
    d_out16 = d_total.astype(jnp.bfloat16)
    g_node_out = matmul(node_act.T, d_out16)
    d_node_pre = (matmul(d_out16, w_node_out.T) * silu_slope(node_pre)).astype(jnp.bfloat16)
    g_node_in = jnp.concatenate([matmul(owned.T, d_node_pre), matmul(summed.T, d_node_pre)], axis=0)
    d_owned = d_total + matmul(d_node_pre, w_node_in[:latent].T)
    d_summed = matmul(d_node_pre, w_node_in[latent:].T).astype(jnp.bfloat16)
    d_message = d_summed[recv_index] * edge_live[:, None].astype(d_summed.dtype)
    g_edge_out = matmul(edge_act.T, d_message)
    d_edge_pre = (matmul(d_message, w_edge_out.T) * silu_slope(edge_pre)).astype(jnp.bfloat16)
    g_edge_in = jnp.concatenate([matmul(senders.T, d_edge_pre), matmul(receivers.T, d_edge_pre)], axis=0)
    d_senders = matmul(d_edge_pre, w_edge_in[:latent].T)
    d_receivers = matmul(d_edge_pre, w_edge_in[latent:].T)
    d_lookup = jax.ops.segment_sum(d_senders, send_index, num_segments=lookup_rows)
    d_owned = d_owned + d_lookup[:rows_here] + jax.ops.segment_sum(d_receivers, recv_index, num_segments=rows_here)
    return d_owned, d_lookup[rows_here:], (g_edge_in, g_edge_out, g_node_in, g_node_out)


def reference(nodes, ghost_rows, ghost_count, edge_send, edge_recv, edge_count, pool_map, w_edge_in, w_edge_out, w_node_in, w_node_out, w_coarse_in, w_coarse_out, d_fine, d_coarse):
    devices = N_GX * N_GY
    latent = nodes.shape[1]
    per_device = nodes.reshape(devices, NODE_DEV, latent)
    d_fine_dev = d_fine.reshape(devices, NODE_DEV, latent)
    weights = (w_edge_in, w_edge_out, w_node_in, w_node_out)
    slot_ids = jnp.arange(GBLK, dtype=jnp.int32)
    edge_ids = jnp.arange(EDGE_DEV, dtype=jnp.int32)
    column_ids = jnp.arange(N_GX, dtype=jnp.int32)
    device_ids = jnp.arange(devices, dtype=jnp.int32)
    direction_ids = jnp.arange(8, dtype=jnp.int32)
    across = jnp.array(offset_across, dtype=jnp.int32)
    along = jnp.array(offset_along, dtype=jnp.int32)

    def halo_of(device):
        column_idx = device // N_GY
        row_idx = device % N_GY
        source_column = column_idx - across
        source_row = row_idx - along
        inside = (source_column >= 0) & (source_column < N_GX) & (source_row >= 0) & (source_row < N_GY)
        sources = jnp.clip(source_column, 0, N_GX - 1) * N_GY + jnp.clip(source_row, 0, N_GY - 1)
        ghost_lists = ghost_rows[sources, direction_ids]
        slot_live = (slot_ids[None, :] < ghost_count[sources, direction_ids][:, None]) & inside[:, None]
        picked = per_device[sources[:, None], ghost_lists]
        picked = jnp.where(slot_live[:, :, None], picked, jnp.zeros_like(picked))
        return picked, sources, ghost_lists, slot_live

    def forward_of(device):
        picked, sources, ghost_lists, slot_live = halo_of(device)
        edge_live = (edge_ids < edge_count[device]).astype(jnp.float32)
        return fine_forward(per_device[device], picked.reshape(8 * GBLK, latent), edge_send[device], edge_recv[device], edge_live, weights), edge_live, sources, ghost_lists, slot_live

    fine_all = lax.map(lambda device: forward_of(device)[0][0], device_ids)
    column_rows = N_GY * CO_DEV

    def parents_of(device):
        return pool_map[device] + (device % N_GY) * CO_DEV - BAND

    def pool_column(column_idx):
        members = column_idx * N_GY + jnp.arange(N_GY, dtype=jnp.int32)

        def one_member(values, member):
            return jax.ops.segment_sum(values.astype(jnp.float32), parents_of(member), num_segments=column_rows)

        parts = jax.vmap(one_member)(fine_all[members], members)
        return (0.125 * jnp.sum(parts, axis=0)).astype(jnp.bfloat16)

    coarse_in = lax.map(pool_column, column_ids).reshape(N_GX * column_rows, latent)
    coarse_pre = matmul(coarse_in, w_coarse_in)
    coarse_act = jax.nn.silu(coarse_pre).astype(jnp.bfloat16)
    coarse_out = (coarse_in.astype(jnp.float32) + matmul(coarse_act, w_coarse_out)).astype(jnp.bfloat16)
    g_coarse_out = matmul(coarse_act.T, d_coarse)
    d_coarse_pre = (matmul(d_coarse, w_coarse_out.T) * silu_slope(coarse_pre)).astype(jnp.bfloat16)
    g_coarse_in = matmul(coarse_in.T, d_coarse_pre)
    d_coarse_in = (d_coarse.astype(jnp.float32) + matmul(d_coarse_pre, w_coarse_in.T)).astype(jnp.bfloat16)
    d_column = d_coarse_in.reshape(N_GX, column_rows, latent)

    def backward_step(carry, device):
        grads_nodes, totals = carry
        outcome, edge_live, sources, ghost_lists, slot_live = forward_of(device)
        stashed = outcome[1]
        column_idx = device // N_GY
        d_total = d_fine_dev[device].astype(jnp.float32) + 0.125 * d_column[column_idx][parents_of(device)].astype(jnp.float32)
        d_owned, d_ghosts, partials = fine_backward(per_device[device], edge_send[device], edge_recv[device], edge_live, weights, stashed, d_total, NODE_DEV + 8 * GBLK)
        rounded = lax.optimization_barrier(d_ghosts.astype(jnp.bfloat16)).astype(jnp.float32).reshape(8, GBLK, latent)
        rounded = jnp.where(slot_live[:, :, None], rounded, jnp.zeros_like(rounded))
        grads_nodes = grads_nodes.at[device].add(d_owned)
        grads_nodes = grads_nodes.at[sources[:, None], ghost_lists].add(rounded)
        totals = tuple(total + term for total, term in zip(totals, partials))
        return (grads_nodes, totals), None

    start_totals = (jnp.zeros((2 * latent, HID), jnp.float32), jnp.zeros((HID, latent), jnp.float32), jnp.zeros((2 * latent, HID), jnp.float32), jnp.zeros((HID, latent), jnp.float32))
    start_grads = jnp.zeros((devices, NODE_DEV, latent), jnp.float32)
    (grads_nodes, totals), unused = lax.scan(backward_step, (start_grads, start_totals), device_ids)
    grad_scale = 1.0 / (NODE_DEV * devices) ** 0.5
    return (fine_all.reshape(devices * NODE_DEV, latent), coarse_out, grads_nodes.reshape(devices * NODE_DEV, latent), totals[0] * grad_scale, totals[1] * grad_scale, totals[2] * grad_scale, totals[3] * grad_scale, g_coarse_in * grad_scale, g_coarse_out * grad_scale)
```

```python
import functools

import jax
import jax.numpy as jnp
from jax import lax
from jax.experimental import pallas as pl
from jax.experimental.pallas import tpu as pltpu
from jax.sharding import PartitionSpec as P

BAND = 32
MESH = pl.DeviceIdType.MESH
ACROSS = (-1, -1, -1, 0, 0, 1, 1, 1)
ALONG = (-1, 0, 1, -1, 1, -1, 0, 1)
SEND_ORDER = (3, 4, 1, 6, 0, 2, 5, 7)
GHOST_ORDER = (1, 6, 3, 4, 0, 2, 5, 7)
F32 = jnp.float32
BF16 = jnp.bfloat16
FOLDS = 4
LANES = 128


def mm(a, b):
    return jnp.dot(a, b, preferred_element_type=F32)


def mm_t(a, b):
    return lax.dot_general(a, b, (((1,), (1,)), ((), ())), preferred_element_type=F32)


def t_mm(a, b):
    return lax.dot_general(a, b, (((0,), (0,)), ((), ())), preferred_element_type=F32)


def sigmoid(v):
    return 1.0 / (1.0 + jnp.exp(-v))


def columns(row):
    return jnp.concatenate(
        [
            jnp.transpose(jnp.broadcast_to(row[:, s : s + LANES], (LANES, LANES)))
            for s in range(0, row.shape[1], LANES)
        ],
        axis=0,
    )


def alive(row, start, count):
    ids = lax.broadcasted_iota(jnp.int32, row.shape, 1) + start
    return jnp.where(ids < count, row, -1)


def pick_lanes(col, width):
    ids = lax.broadcasted_iota(jnp.int32, (col.shape[0], LANES), 1)
    parts = [
        jnp.where(ids == col - s, 1.0, 0.0).astype(BF16)[:, : min(LANES, width - s)]
        for s in range(0, width, LANES)
    ]
    return jnp.concatenate(parts, axis=1)


def pick_sublanes(row, height):
    ids = lax.broadcasted_iota(jnp.int32, (height, row.shape[1]), 0)
    return jnp.where(ids == row, 1.0, 0.0).astype(BF16)


def choose(block, first, wide):
    width = wide.shape[1] // FOLDS
    out = jnp.zeros((wide.shape[0], width), F32)
    for j in range(FOLDS):
        out = jnp.where(block == first + j, wide[:, j * width : (j + 1) * width], out)
    return out


def spread(values, fold):
    values = values.astype(F32)
    return jnp.concatenate(
        [jnp.where(fold == j, values, 0.0).astype(BF16) for j in range(FOLDS)], axis=1
    )


def slope(s, v):
    return s * (1.0 + v * (1.0 - s))


def neighbours(n_gx, n_gy, sign):
    a, b = lax.axis_index("gx"), lax.axis_index("gy")
    found = []
    for dx, dy in zip(ACROSS, ALONG):
        dx, dy = sign * dx, sign * dy
        ta, tb = a + dx, b + dy
        sa, sb = a - dx, b - dy
        there = (ta >= 0) & (ta < n_gx) & (tb >= 0) & (tb < n_gy)
        here = (sa >= 0) & (sa < n_gx) & (sb >= 0) & (sb < n_gy)
        target = (jnp.clip(ta, 0, n_gx - 1), jnp.clip(tb, 0, n_gy - 1))
        found.append((target, there, here))
    return found


def remote(src, dst, send, recv, peer):
    return pltpu.make_async_remote_copy(
        src_ref=src, dst_ref=dst, send_sem=send, recv_sem=recv, device_id=peer, device_id_type=MESH)


def exchange_copies(found, src_ref, dst_ref, send_sem, recv_sem):
    return [
        remote(src_ref.at[k], dst_ref.at[k], send_sem.at[k], recv_sem.at[k], found[k][0])
        for k in range(len(found))
    ]


def clear_absent(found, dst_ref):
    for k in range(len(found)):
        @pl.when(jnp.logical_not(found[k][2]))
        def _(k=k):
            dst_ref[k] = jnp.zeros(dst_ref.shape[1:], dst_ref.dtype)


def start(found, copies, k):
    @pl.when(found[k][1])
    def _():
        copies[k].start()


def wait_recv(found, copies, k):
    @pl.when(found[k][2])
    def _():
        copies[k].wait_recv()


def wait_sends(found, copies):
    for k in range(len(found)):
        @pl.when(found[k][1])
        def _(k=k):
            copies[k].wait_send()


class Rims:
    def __init__(self, n_gy, low, high, got, send_sem, recv_sem):
        a, b = lax.axis_index("gx"), lax.axis_index("gy")
        self.below, self.above = b > 0, b < n_gy - 1
        self.down = remote(low, got.at[1], send_sem.at[0], recv_sem.at[1], (a, jnp.maximum(b - 1, 0)))
        self.up = remote(high, got.at[0], send_sem.at[1], recv_sem.at[0], (a, jnp.minimum(b + 1, n_gy - 1)))
        self.got = got

    def start(self):
        @pl.when(self.below)
        def _():
            self.down.start()

        @pl.when(self.above)
        def _():
            self.up.start()

        for slot, there in ((0, self.below), (1, self.above)):
            @pl.when(jnp.logical_not(there))
            def _(slot=slot):
                self.got[slot] = jnp.zeros(self.got.shape[1:], self.got.dtype)

    def wait(self):
        @pl.when(self.below)
        def _():
            self.up.wait_recv()

        @pl.when(self.above)
        def _():
            self.down.wait_recv()

    def drain(self):
        @pl.when(self.below)
        def _():
            self.down.wait_send()

        @pl.when(self.above)
        def _():
            self.up.wait_send()


class Total:
    def __init__(self, peers_x, peers_y, total, g16, got_x, got_y, mine, xs, xr, ys, yr, zs, zr):
        a, b = lax.axis_index("gx"), lax.axis_index("gy")
        self.n_gy = len(peers_y) + 1
        self.total, self.g16, self.got_x, self.got_y, self.mine = total, g16, got_x, got_y, mine
        self.first = [remote(g16.at[p[0]], got_x.at[r], xs.at[r], xr.at[r], p) for r, p in enumerate(peers_x)]
        self.second = [
            remote(got_y.at[0], got_y.at[r + 1], ys.at[r], yr.at[r], p) for r, p in enumerate(peers_y)
        ]
        self.third = [remote(mine, total.at[a], zs.at[r], zr.at[r], p) for r, p in enumerate(peers_x)]

    def load(self, parts):
        flat = jnp.concatenate(parts, axis=0).astype(BF16)
        share = self.g16.shape[1]
        for i in range(self.g16.shape[0]):
            self.g16[i] = flat[i * share : (i + 1) * share]
        for copy in self.first:
            copy.start()

    def across(self):
        acc = self.g16[lax.axis_index("gx")].astype(F32)
        for r, copy in enumerate(self.first):
            copy.wait_recv()
            acc = acc + self.got_x[r].astype(F32)
        self.got_y[0] = acc.astype(BF16)
        for copy in self.second:
            copy.start()

    def along(self):
        a, b = lax.axis_index("gx"), lax.axis_index("gy")
        for copy in self.second:
            copy.wait_recv()
        acc = jnp.zeros(self.mine.shape, F32)
        for y in range(self.n_gy):
            acc = acc + self.got_y[lax.rem(b - y + self.n_gy, self.n_gy)].astype(F32)
        self.mine[...] = acc.astype(BF16)
        for copy in self.third:
            copy.start()
        self.total[a] = acc.astype(BF16)

    def finish(self):
        for copy in self.third:
            copy.wait_recv()
        for copy in self.first + self.second + self.third:
            copy.wait_send()


def main_kernel(
    n_gx, n_gy, chunk,
    nodes_ref, rows_ref, gcount_ref, send_ref, recv_ref, ecount_ref, pool_ref,
    wei_ref, weo_ref, wni_ref, wno_ref, wci_ref, wco_ref, d_fine_ref, d_coarse_ref,
    fine_ref, coarse_ref, grad_ref, early_ref, late_ref,
    outgoing, arrived, back_out, back, nodes_wide, ghost_wide, ghost_block,
    srow, rrow, s_block, r_block, s_lanes, r_lanes, r_rows, s_rows, g_rows,
    pairs, act_ref, slope_ref, wide_r, wide_s, both, node_slope,
    rims, got_rims, got_dc, g_in, g_out,
    e16, e_x, e_y, e_mine, l16, l_x, l_y, l_mine,
    out_s, out_r, ret_s, ret_r, rim_s, rim_r,
    exs, exr, eys, eyr, ezs, ezr, lxs, lxr, lys, lyr, lzs, lzr,
):
    rows, latent = nodes_ref.shape
    edges_n = send_ref.shape[1]
    peers, slots = rows_ref.shape[1:]
    co = d_coarse_ref.shape[0]
    bits = slots.bit_length() - 1
    own = rows // slots
    a, b = lax.axis_index("gx"), lax.axis_index("gy")
    found = neighbours(n_gx, n_gy, 1)
    returns = neighbours(n_gx, n_gy, -1)
    peers_x = [(lax.rem(a + r, n_gx), b) for r in range(1, n_gx)]
    peers_y = [(a, lax.rem(b + r, n_gy)) for r in range(1, n_gy)]
    corners = [f for f, dx, dy in zip(found, ACROSS, ALONG) if dx and dy]

    barrier = pltpu.get_barrier_semaphore()
    expect = jnp.int32(n_gx + n_gy - 2)
    for target, there, _ in corners:
        @pl.when(there)
        def _(target=target):
            pl.semaphore_signal(barrier, inc=1, device_id=target, device_id_type=MESH)
        expect = expect + jnp.where(there, 1, 0)
    for peer in peers_x + peers_y:
        pl.semaphore_signal(barrier, inc=1, device_id=peer, device_id_type=MESH)

    sent = exchange_copies(found, outgoing, arrived, out_s, out_r)
    returned = exchange_copies(returns, back_out, back, ret_s, ret_r)
    dc_rims = Rims(n_gy, d_coarse_ref.at[:BAND], d_coarse_ref.at[co - BAND :], got_dc, rim_s.at[0], rim_r.at[0])
    pool_rims = Rims(n_gy, rims.at[0], rims.at[1], got_rims, rim_s.at[1], rim_r.at[1])
    early = Total(peers_x, peers_y, early_ref, e16, e_x, e_y, e_mine, exs, exr, eys, eyr, ezs, ezr)
    late = Total(peers_x, peers_y, late_ref, l16, l_x, l_y, l_mine, lxs, lxr, lys, lyr, lzs, lzr)

    def ghost_row(k):
        return alive(rows_ref[0, k : k + 1, :], 0, gcount_ref[:, k : k + 1])

    for j in range(own):
        nodes_wide[:, j * latent : (j + 1) * latent] = nodes_ref[j * slots : (j + 1) * slots]
    for n, k in enumerate(SEND_ORDER):
        col = columns(ghost_row(k))
        block = col >> bits
        ghost_block[k] = block
        outgoing[k] = choose(block, 0, mm(pick_lanes(col & (slots - 1), slots), nodes_wide[...])).astype(BF16)
        if n == 0:
            pl.semaphore_wait(barrier, expect)
        start(found, sent, k)
    dc_rims.start()
    clear_absent(found, arrived)
    clear_absent(returns, back)

    send = send_ref[...]
    moved = send
    for place, k in enumerate(GHOST_ORDER):
        moved = jnp.where((send >> bits) == own + k, (send & (slots - 1)) + ((own + place) << bits), moved)
    srow[...] = moved
    rrow[...] = alive(recv_ref[...], 0, ecount_ref[0])

    def first_pass(i, carry):
        at = pl.ds(pl.multiple_of(i * chunk, chunk), chunk)
        s_col, r_col = columns(srow[:, at]), columns(rrow[:, at])
        s_blk, r_blk = s_col >> bits, r_col >> bits
        s_block[at, :] = s_blk
        r_block[at, :] = r_blk
        s_hot, r_hot = pick_lanes(s_col & (slots - 1), slots), pick_lanes(r_col & (slots - 1), slots)
        s_lanes[at, :] = s_hot
        r_lanes[at, :] = r_hot
        pairs[at, :latent] = choose(s_blk, 0, mm(s_hot, nodes_wide[...])).astype(BF16)
        pairs[at, latent:] = choose(r_blk, 0, mm(r_hot, nodes_wide[...])).astype(BF16)
        return carry

    steps = edges_n // chunk
    lax.fori_loop(0, steps, first_pass, 0)

    def hot_rows(i, carry):
        at = pl.ds(pl.multiple_of(i * chunk, chunk), chunk)
        s, r = srow[:, at], rrow[:, at]
        r_rows[:, at] = pick_sublanes(r & (slots - 1), slots)
        for t in range(s_rows.shape[0]):
            s_rows[t, :, at] = pick_sublanes(
                jnp.where((s >> bits) // FOLDS == t, s & (slots - 1), -1), slots)
        return carry

    lax.fori_loop(0, steps, hot_rows, 0)
    for k in range(peers):
        g_rows[:, k * slots : (k + 1) * slots] = pick_sublanes(ghost_row(k) & (slots - 1), slots)

    def take_ghosts(group):
        for j, k in enumerate(GHOST_ORDER[group * FOLDS : (group + 1) * FOLDS]):
            wait_recv(found, sent, k)
        for j, k in enumerate(GHOST_ORDER[group * FOLDS : (group + 1) * FOLDS]):
            ghost_wide[:, j * latent : (j + 1) * latent] = arrived[k]

    take_ghosts(0)

    def second_pass(i, carry):
        at = pl.ds(pl.multiple_of(i * chunk, chunk), chunk)
        got = choose(s_block[at, :], own, mm(s_lanes[at, :], ghost_wide[...])).astype(BF16)
        pairs[at, :latent] = pairs[at, :latent] + got
        return carry

    lax.fori_loop(0, steps, second_pass, 0)
    take_ghosts(1)

    def third_pass(i, carry):
        at = pl.ds(pl.multiple_of(i * chunk, chunk), chunk)
        got = choose(s_block[at, :], own + FOLDS, mm(s_lanes[at, :], ghost_wide[...])).astype(BF16)
        pairs[at, :latent] = pairs[at, :latent] + got
        pre = mm(pairs[at, :], wei_ref[...])
        s = sigmoid(pre)
        act = (pre * s).astype(BF16)
        act_ref[at, :] = act
        slope_ref[at, :] = slope(s, pre)
        wide_r[at, :] = spread(mm(act, weo_ref[...]).astype(BF16), r_block[at, :])
        return carry

    lax.fori_loop(0, steps, third_pass, 0)

    both[:, :latent] = nodes_ref[...]
    summed = mm(r_rows[...], wide_r[...])
    for j in range(FOLDS):
        both[j * slots : (j + 1) * slots, latent:] = summed[:, j * latent : (j + 1) * latent].astype(BF16)
    node_pre = mm(both[...], wni_ref[...])
    s = sigmoid(node_pre)
    node_act = (node_pre * s).astype(BF16)
    node_slope[...] = slope(s, node_pre)
    fine = (nodes_ref[...].astype(F32) + mm(node_act, wno_ref[...])).astype(BF16)
    fine_ref[...] = fine
    window = mm(pick_sublanes(pool_ref[...], co + 2 * BAND), fine)
    rims[0] = window[: 2 * BAND].astype(BF16)
    rims[1] = window[co:].astype(BF16)
    pool_rims.start()

    dc_rims.wait()
    d_coarse = d_coarse_ref[...]
    d_wide = jnp.concatenate([got_dc[0], d_coarse, got_dc[1]], axis=0)
    d_act = mm_t(d_wide, wco_ref[...])
    pool_hot = pick_lanes(columns(pool_ref[...]), co + 2 * BAND)
    pool_rims.wait()
    coarse_in = (0.125 * jnp.concatenate(
        [
            window[: 2 * BAND] + got_rims[0].astype(F32),
            window[2 * BAND : co],
            window[co:] + got_rims[1].astype(F32),
        ],
        axis=0,
    )).astype(BF16)
    pre = mm(coarse_in, wci_ref[...])
    s = sigmoid(pre)
    d_pre = (d_act * slope(s, pre)).astype(BF16)
    reach = (d_wide.astype(F32) + mm_t(d_pre, wci_ref[...])).astype(BF16)

    d_total = d_fine_ref[...].astype(F32) + 0.125 * mm(pool_hot, reach)
    d16 = d_total.astype(BF16)
    d_node = (mm_t(d16, wno_ref[...]) * node_slope[...]).astype(BF16)
    d_summed = mm_t(d_node, wni_ref[latent:, :]).astype(BF16)
    for j in range(FOLDS):
        ghost_wide[:, j * latent : (j + 1) * latent] = d_summed[j * slots : (j + 1) * slots]
    grad_ref[...] = d_total + mm_t(d_node, wni_ref[:latent, :])
    mid = slice(BAND, co + BAND)
    act = (pre * s)[mid].astype(BF16)
    coarse_ref[...] = (coarse_in[mid].astype(F32) + mm(act, wco_ref[...])).astype(BF16)
    early.load([
        t_mm(both[...], d_node), t_mm(node_act, d16), t_mm(coarse_in[mid], d_pre[mid]), t_mm(act, d_coarse)])
    g_in[...] = jnp.zeros_like(g_in)
    g_out[...] = jnp.zeros_like(g_out)

    def back_pass(i, carry):
        at = pl.ds(pl.multiple_of(i * chunk, chunk), chunk)
        r_blk = r_block[at, :]
        d_message = choose(r_blk, 0, mm(r_lanes[at, :], ghost_wide[...])).astype(BF16)
        g_out[...] += t_mm(act_ref[at, :], d_message)
        d_edge = (mm_t(d_message, weo_ref[...]) * slope_ref[at, :]).astype(BF16)
        g_in[...] += t_mm(pairs[at, :], d_edge)
        wide_r[at, :] = spread(d_edge, r_blk)
        wide_s[at, :] = spread(d_edge, s_block[at, :] & (FOLDS - 1))
        return carry

    lax.fori_loop(0, steps, back_pass, 0)
    late.load([g_in[...], g_out[...]])
    early.across()

    w_send, w_recv = wei_ref[:latent, :], wei_ref[latent:, :]

    def give_ghosts(group):
        sums = mm(s_rows[1 + group], wide_s[...]).astype(BF16)
        for j, k in enumerate(GHOST_ORDER[group * FOLDS : (group + 1) * FOLDS]):
            back_out[k] = mm_t(sums[:, j * latent : (j + 1) * latent], w_send).astype(BF16)
            start(returns, returned, k)

    give_ghosts(1)
    give_ghosts(0)
    late.across()
    early.along()
    sums_s = mm(s_rows[0], wide_s[...]).astype(BF16)
    sums_r = mm(r_rows[...], wide_r[...]).astype(BF16)
    for j in range(FOLDS):
        at = slice(j * slots, (j + 1) * slots)
        lanes = slice(j * latent, (j + 1) * latent)
        grad_ref[at, :] += mm_t(sums_s[:, lanes], w_send) + mm_t(sums_r[:, lanes], w_recv)
    late.along()
    for k in range(peers):
        wait_recv(returns, returned, k)
        wide_s[k * slots : (k + 1) * slots, :] = spread(back[k], ghost_block[k])
    sums_g = mm(g_rows[...], wide_s[: peers * slots, :])
    for j in range(FOLDS):
        grad_ref[j * slots : (j + 1) * slots, :] += sums_g[:, j * latent : (j + 1) * latent]
    early.finish()
    late.finish()
    wait_sends(found, sent)
    wait_sends(returns, returned)
    dc_rims.drain()
    pool_rims.drain()


def final_kernel(
    scale, fine_in, coarse_in, grad_in, early_in, late_in,
    fine_out, coarse_out, grad_out, ei_ref, eo_ref, ni_ref, no_ref, ci_ref, co_ref,
):
    fine_out[...] = fine_in[...]
    coarse_out[...] = coarse_in[...]
    grad_out[...] = grad_in[...]

    def put(total_ref, refs):
        flat = total_ref[...].reshape(-1, total_ref.shape[-1]).astype(F32) * scale
        at = 0
        for ref in refs:
            ref[...] = flat[at : at + ref.shape[0]]
            at += ref.shape[0]

    put(early_in, (ni_ref, no_ref, ci_ref, co_ref))
    put(late_in, (ei_ref, eo_ref))


def body(
    n_gx, n_gy, nodes, ghost_rows, ghost_count, edge_send, edge_recv, edge_count, pool_map,
    w_edge_in, w_edge_out, w_node_in, w_node_out, w_coarse_in, w_coarse_out, d_fine, d_coarse,
):
    rows, latent = nodes.shape
    _, peers, slots = ghost_rows.shape
    edges_n = edge_send.shape[1]
    co = d_coarse.shape[0]
    chunk = 512 if edges_n % 512 == 0 else edges_n
    groups = (rows // slots + peers) // FOLDS
    dma = pltpu.SemaphoreType.DMA
    vmem = pl.BlockSpec(memory_space=pltpu.VMEM)
    smem = pl.BlockSpec(memory_space=pltpu.SMEM)
    early_rows, late_rows = 5 * latent // n_gx, 3 * latent // n_gx

    def total_buffers(share):
        return [
            pltpu.VMEM((n_gx, share, latent), BF16), pltpu.VMEM((n_gx - 1, share, latent), BF16),
            pltpu.VMEM((n_gy, share, latent), BF16), pltpu.VMEM((share, latent), BF16)]

    total_sems = [dma((n_gx - 1,))] * 2 + [dma((n_gy - 1,))] * 2 + [dma((n_gx - 1,))] * 2
    halo = pltpu.VMEM((peers, slots, latent), BF16)
    results = pl.pallas_call(
        functools.partial(main_kernel, n_gx, n_gy, chunk),
        out_shape=[
            jax.ShapeDtypeStruct((rows, latent), BF16), jax.ShapeDtypeStruct((co, latent), BF16),
            jax.ShapeDtypeStruct((rows, latent), F32),
            jax.ShapeDtypeStruct((n_gx, early_rows, latent), BF16),
            jax.ShapeDtypeStruct((n_gx, late_rows, latent), BF16)],
        in_specs=[vmem] * 5 + [smem] + [vmem] * 9,
        out_specs=[vmem] * 5,
        scratch_shapes=[halo] * 4 + [
            pltpu.VMEM((slots, FOLDS * latent), BF16), pltpu.VMEM((slots, FOLDS * latent), BF16),
            pltpu.VMEM((peers, slots, LANES), jnp.int32),
            pltpu.VMEM((1, edges_n), jnp.int32), pltpu.VMEM((1, edges_n), jnp.int32),
            pltpu.VMEM((edges_n, LANES), jnp.int32), pltpu.VMEM((edges_n, LANES), jnp.int32),
            pltpu.VMEM((edges_n, slots), BF16), pltpu.VMEM((edges_n, slots), BF16),
            pltpu.VMEM((slots, edges_n), BF16), pltpu.VMEM((groups, slots, edges_n), BF16),
            pltpu.VMEM((slots, peers * slots), BF16),
            pltpu.VMEM((edges_n, 2 * latent), BF16), pltpu.VMEM((edges_n, latent), BF16),
            pltpu.VMEM((edges_n, latent), F32),
            pltpu.VMEM((edges_n, FOLDS * latent), BF16), pltpu.VMEM((edges_n, FOLDS * latent), BF16),
            pltpu.VMEM((rows, 2 * latent), BF16), pltpu.VMEM((rows, latent), F32),
            pltpu.VMEM((2, 2 * BAND, latent), BF16), pltpu.VMEM((2, 2 * BAND, latent), BF16),
            pltpu.VMEM((2, BAND, latent), BF16),
            pltpu.VMEM((2 * latent, latent), F32), pltpu.VMEM((latent, latent), F32),
        ] + total_buffers(early_rows) + total_buffers(late_rows)
        + [dma((peers,))] * 4 + [dma((2, 2))] * 2 + total_sems * 2,
        compiler_params=pltpu.CompilerParams(
            vmem_limit_bytes=48 * 1024 * 1024, collective_id=0, has_side_effects=True),
    )(nodes, ghost_rows, ghost_count, edge_send, edge_recv, edge_count, pool_map,
      w_edge_in, w_edge_out, w_node_in, w_node_out, w_coarse_in, w_coarse_out, d_fine, d_coarse)
    scale = 1.0 / (rows * n_gx * n_gy) ** 0.5
    fine, coarse, grads, ei, eo, ni, no, ci, co_grad = pl.pallas_call(
        functools.partial(final_kernel, scale),
        out_shape=[
            jax.ShapeDtypeStruct((rows, latent), BF16), jax.ShapeDtypeStruct((co, latent), BF16),
            jax.ShapeDtypeStruct((rows, latent), F32)] + [
            jax.ShapeDtypeStruct((n * latent, latent), F32) for n in (2, 1, 2, 1, 1, 1)],
        in_specs=[vmem] * 5,
        out_specs=[vmem] * 9,
        compiler_params=pltpu.CompilerParams(vmem_limit_bytes=8 * 1024 * 1024),
    )(*results)
    return fine, coarse, grads, ei, eo, ni, no, ci, co_grad


def solution(mesh):
    split = P(("gx", "gy"), None)
    return jax.shard_map(
        functools.partial(body, mesh.shape["gx"], mesh.shape["gy"]),
        mesh=mesh,
        in_specs=(split, P(("gx", "gy"), None, None), split, split, split, P(("gx", "gy")), split)
        + (P(),) * 6
        + (split, split),
        out_specs=(split, split, split) + (P(),) * 6,
        check_vma=False,
    )
```

```python
import functools

import jax
import jax.numpy as jnp
from jax import lax
from jax.experimental import pallas as pl
from jax.experimental.pallas import tpu as pltpu
from jax.sharding import PartitionSpec as P

BAND = 32
MESH = pl.DeviceIdType.MESH
ACROSS = (-1, -1, -1, 0, 0, 1, 1, 1)
ALONG = (-1, 0, 1, -1, 1, -1, 0, 1)
SEND_ORDER = (3, 4, 1, 6, 0, 2, 5, 7)
GHOST_ORDER = (1, 6, 3, 4, 0, 2, 5, 7)
F32 = jnp.float32
BF16 = jnp.bfloat16
FOLDS = 4
LANES = 128


def mm(a, b):
    return jnp.dot(a, b, preferred_element_type=F32)


def mm_t(a, b):
    return lax.dot_general(a, b, (((1,), (1,)), ((), ())), preferred_element_type=F32)


def t_mm(a, b):
    return lax.dot_general(a, b, (((0,), (0,)), ((), ())), preferred_element_type=F32)


def sigmoid(v):
    return 1.0 / (1.0 + jnp.exp(-v))


def columns(row):
    return jnp.concatenate(
        [
            jnp.transpose(jnp.broadcast_to(row[:, s : s + LANES], (LANES, LANES)))
            for s in range(0, row.shape[1], LANES)
        ],
        axis=0,
    )


def alive(row, start, count):
    ids = lax.broadcasted_iota(jnp.int32, row.shape, 1) + start
    return jnp.where(ids < count, row, -1)


def pick_lanes(col, width):
    ids = lax.broadcasted_iota(jnp.int32, (col.shape[0], LANES), 1)
    parts = [
        jnp.where(ids == col - s, 1.0, 0.0).astype(BF16)[:, : min(LANES, width - s)]
        for s in range(0, width, LANES)
    ]
    return jnp.concatenate(parts, axis=1)


def pick_sublanes(row, height):
    ids = lax.broadcasted_iota(jnp.int32, (height, row.shape[1]), 0)
    return jnp.where(ids == row, 1.0, 0.0).astype(BF16)


def choose(block, first, wide):
    width = wide.shape[1] // FOLDS
    out = jnp.zeros((wide.shape[0], width), F32)
    for j in range(FOLDS):
        out = jnp.where(block == first + j, wide[:, j * width : (j + 1) * width], out)
    return out


def spread(values, fold):
    values = values.astype(F32)
    return jnp.concatenate(
        [jnp.where(fold == j, values, 0.0).astype(BF16) for j in range(FOLDS)], axis=1
    )


def slope(s, v):
    return s * (1.0 + v * (1.0 - s))


def neighbours(n_gx, n_gy, sign):
    a, b = lax.axis_index("gx"), lax.axis_index("gy")
    found = []
    for dx, dy in zip(ACROSS, ALONG):
        dx, dy = sign * dx, sign * dy
        ta, tb = a + dx, b + dy
        sa, sb = a - dx, b - dy
        there = (ta >= 0) & (ta < n_gx) & (tb >= 0) & (tb < n_gy)
        here = (sa >= 0) & (sa < n_gx) & (sb >= 0) & (sb < n_gy)
        target = (jnp.clip(ta, 0, n_gx - 1), jnp.clip(tb, 0, n_gy - 1))
        found.append((target, there, here))
    return found


def remote(src, dst, send, recv, peer):
    return pltpu.make_async_remote_copy(
        src_ref=src, dst_ref=dst, send_sem=send, recv_sem=recv, device_id=peer, device_id_type=MESH)


def exchange_copies(found, src_ref, dst_ref, send_sem, recv_sem):
    return [
        remote(src_ref.at[k], dst_ref.at[k], send_sem.at[k], recv_sem.at[k], found[k][0])
        for k in range(len(found))
    ]


def clear_absent(found, dst_ref):
    for k in range(len(found)):
        @pl.when(jnp.logical_not(found[k][2]))
        def _(k=k):
            dst_ref[k] = jnp.zeros(dst_ref.shape[1:], dst_ref.dtype)


def start(found, copies, k):
    @pl.when(found[k][1])
    def _():
        copies[k].start()


def wait_recv(found, copies, k):
    @pl.when(found[k][2])
    def _():
        copies[k].wait_recv()


def wait_sends(found, copies):
    for k in range(len(found)):
        @pl.when(found[k][1])
        def _(k=k):
            copies[k].wait_send()


class Rims:
    def __init__(self, n_gy, low, high, got, send_sem, recv_sem):
        a, b = lax.axis_index("gx"), lax.axis_index("gy")
        self.below, self.above = b > 0, b < n_gy - 1
        self.down = remote(low, got.at[1], send_sem.at[0], recv_sem.at[1], (a, jnp.maximum(b - 1, 0)))
        self.up = remote(high, got.at[0], send_sem.at[1], recv_sem.at[0], (a, jnp.minimum(b + 1, n_gy - 1)))
        self.got = got

    def start(self):
        @pl.when(self.below)
        def _():
            self.down.start()

        @pl.when(self.above)
        def _():
            self.up.start()

        for slot, there in ((0, self.below), (1, self.above)):
            @pl.when(jnp.logical_not(there))
            def _(slot=slot):
                self.got[slot] = jnp.zeros(self.got.shape[1:], self.got.dtype)

    def wait(self):
        @pl.when(self.below)
        def _():
            self.up.wait_recv()

        @pl.when(self.above)
        def _():
            self.down.wait_recv()

    def drain(self):
        @pl.when(self.below)
        def _():
            self.down.wait_send()

        @pl.when(self.above)
        def _():
            self.up.wait_send()


class Total:
    def __init__(self, peers_x, peers_y, total, g16, got_x, got_y, mine, xs, xr, ys, yr, zs, zr):
        a, b = lax.axis_index("gx"), lax.axis_index("gy")
        self.n_gy = len(peers_y) + 1
        self.total, self.g16, self.got_x, self.got_y, self.mine = total, g16, got_x, got_y, mine
        self.first = [remote(g16.at[p[0]], got_x.at[r], xs.at[r], xr.at[r], p) for r, p in enumerate(peers_x)]
        self.second = [
            remote(got_y.at[0], got_y.at[r + 1], ys.at[r], yr.at[r], p) for r, p in enumerate(peers_y)
        ]
        self.third = [remote(mine, total.at[a], zs.at[r], zr.at[r], p) for r, p in enumerate(peers_x)]

    def load(self, parts):
        flat = jnp.concatenate(parts, axis=0).astype(BF16)
        share = self.g16.shape[1]
        for i in range(self.g16.shape[0]):
            self.g16[i] = flat[i * share : (i + 1) * share]
        for copy in self.first:
            copy.start()

    def across(self):
        acc = self.g16[lax.axis_index("gx")].astype(F32)
        for r, copy in enumerate(self.first):
            copy.wait_recv()
            acc = acc + self.got_x[r].astype(F32)
        self.got_y[0] = acc.astype(BF16)
        for copy in self.second:
            copy.start()

    def along(self):
        a, b = lax.axis_index("gx"), lax.axis_index("gy")
        for copy in self.second:
            copy.wait_recv()
        acc = jnp.zeros(self.mine.shape, F32)
        for y in range(self.n_gy):
            acc = acc + self.got_y[lax.rem(b - y + self.n_gy, self.n_gy)].astype(F32)
        self.mine[...] = acc.astype(BF16)
        for copy in self.third:
            copy.start()
        self.total[a] = acc.astype(BF16)

    def finish(self):
        for copy in self.third:
            copy.wait_recv()
        for copy in self.first + self.second + self.third:
            copy.wait_send()


def main_kernel(
    n_gx, n_gy, chunk,
    ecount_ref, nodes_in, rows_in, gcount_in, send_in, recv_in, pool_in,
    wei_in, weo_in, wni_in, wno_in, wci_in, wco_in, d_fine_in, d_coarse_in,
    fine_ref, coarse_ref, grad_ref, early_ref, late_ref,
    nodes_ref, rows_ref, gcount_ref, send_ref, recv_ref, pool_ref,
    wei_ref, weo_ref, wni_ref, wno_ref, wci_ref, wco_ref, d_fine_ref, d_coarse_ref, load_sem,
    outgoing, arrived, back_out, back, nodes_wide, ghost_wide, ghost_block,
    srow, rrow, s_block, r_block, s_lanes, r_lanes, r_rows, s_rows, g_rows,
    pairs, act_ref, slope_ref, wide_r, wide_s, both, node_slope,
    rims, got_rims, got_dc, g_in, g_out,
    e16, e_x, e_y, e_mine, l16, l_x, l_y, l_mine,
    out_s, out_r, ret_s, ret_r, rim_s, rim_r,
    exs, exr, eys, eyr, ezs, ezr, lxs, lxr, lys, lyr, lzs, lzr,
):
    rows, latent = nodes_ref.shape
    edges_n = send_ref.shape[1]
    peers, slots = rows_ref.shape[1:]
    co = d_coarse_ref.shape[0]
    bits = slots.bit_length() - 1
    own = rows // slots
    a, b = lax.axis_index("gx"), lax.axis_index("gy")
    found = neighbours(n_gx, n_gy, 1)
    returns = neighbours(n_gx, n_gy, -1)
    peers_x = [(lax.rem(a + r, n_gx), b) for r in range(1, n_gx)]
    peers_y = [(a, lax.rem(b + r, n_gy)) for r in range(1, n_gy)]
    corners = [f for f, dx, dy in zip(found, ACROSS, ALONG) if dx and dy]

    loads = [
        pltpu.make_async_copy(src, dst, load_sem.at[i])
        for i, (src, dst) in enumerate((
            (rows_in, rows_ref), (gcount_in, gcount_ref), (nodes_in, nodes_ref), (d_coarse_in, d_coarse_ref),
            (send_in, send_ref), (recv_in, recv_ref), (wei_in, wei_ref), (weo_in, weo_ref), (wni_in, wni_ref),
            (wno_in, wno_ref), (pool_in, pool_ref), (wco_in, wco_ref), (wci_in, wci_ref), (d_fine_in, d_fine_ref)))
    ]
    for load in loads:
        load.start()
    barrier = pltpu.get_barrier_semaphore()
    expect = jnp.int32(n_gx + n_gy - 2)
    for target, there, _ in corners:
        @pl.when(there)
        def _(target=target):
            pl.semaphore_signal(barrier, inc=1, device_id=target, device_id_type=MESH)
        expect = expect + jnp.where(there, 1, 0)
    for peer in peers_x + peers_y:
        pl.semaphore_signal(barrier, inc=1, device_id=peer, device_id_type=MESH)

    sent = exchange_copies(found, outgoing, arrived, out_s, out_r)
    returned = exchange_copies(returns, back_out, back, ret_s, ret_r)
    dc_rims = Rims(n_gy, d_coarse_ref.at[:BAND], d_coarse_ref.at[co - BAND :], got_dc, rim_s.at[0], rim_r.at[0])
    pool_rims = Rims(n_gy, rims.at[0], rims.at[1], got_rims, rim_s.at[1], rim_r.at[1])
    early = Total(peers_x, peers_y, early_ref, e16, e_x, e_y, e_mine, exs, exr, eys, eyr, ezs, ezr)
    late = Total(peers_x, peers_y, late_ref, l16, l_x, l_y, l_mine, lxs, lxr, lys, lyr, lzs, lzr)

    def ghost_row(k):
        return alive(rows_ref[0, k : k + 1, :], 0, gcount_ref[:, k : k + 1])

    for load in loads[:3]:
        load.wait()
    for j in range(own):
        nodes_wide[:, j * latent : (j + 1) * latent] = nodes_ref[j * slots : (j + 1) * slots]
    for n, k in enumerate(SEND_ORDER):
        col = columns(ghost_row(k))
        block = col >> bits
        ghost_block[k] = block
        outgoing[k] = choose(block, 0, mm(pick_lanes(col & (slots - 1), slots), nodes_wide[...])).astype(BF16)
        if n == 0:
            pl.semaphore_wait(barrier, expect)
        start(found, sent, k)
    for load in loads[3:]:
        load.wait()
    dc_rims.start()
    clear_absent(found, arrived)
    clear_absent(returns, back)

    send = send_ref[...]
    moved = send
    for place, k in enumerate(GHOST_ORDER):
        moved = jnp.where((send >> bits) == own + k, (send & (slots - 1)) + ((own + place) << bits), moved)
    srow[...] = moved
    rrow[...] = alive(recv_ref[...], 0, ecount_ref[0])

    def first_pass(i, carry):
        at = pl.ds(pl.multiple_of(i * chunk, chunk), chunk)
        s_col, r_col = columns(srow[:, at]), columns(rrow[:, at])
        s_blk, r_blk = s_col >> bits, r_col >> bits
        s_block[at, :] = s_blk
        r_block[at, :] = r_blk
        s_hot, r_hot = pick_lanes(s_col & (slots - 1), slots), pick_lanes(r_col & (slots - 1), slots)
        s_lanes[at, :] = s_hot
        r_lanes[at, :] = r_hot
        pairs[at, :latent] = choose(s_blk, 0, mm(s_hot, nodes_wide[...])).astype(BF16)
        pairs[at, latent:] = choose(r_blk, 0, mm(r_hot, nodes_wide[...])).astype(BF16)
        return carry

    steps = edges_n // chunk
    lax.fori_loop(0, steps, first_pass, 0)

    def hot_rows(i, carry):
        at = pl.ds(pl.multiple_of(i * chunk, chunk), chunk)
        s, r = srow[:, at], rrow[:, at]
        r_rows[:, at] = pick_sublanes(r & (slots - 1), slots)
        for t in range(s_rows.shape[0]):
            s_rows[t, :, at] = pick_sublanes(
                jnp.where((s >> bits) // FOLDS == t, s & (slots - 1), -1), slots)
        return carry

    lax.fori_loop(0, steps, hot_rows, 0)
    for k in range(peers):
        g_rows[:, k * slots : (k + 1) * slots] = pick_sublanes(ghost_row(k) & (slots - 1), slots)

    def take_ghosts(group):
        for j, k in enumerate(GHOST_ORDER[group * FOLDS : (group + 1) * FOLDS]):
            wait_recv(found, sent, k)
        for j, k in enumerate(GHOST_ORDER[group * FOLDS : (group + 1) * FOLDS]):
            ghost_wide[:, j * latent : (j + 1) * latent] = arrived[k]

    take_ghosts(0)

    def second_pass(i, carry):
        at = pl.ds(pl.multiple_of(i * chunk, chunk), chunk)
        got = choose(s_block[at, :], own, mm(s_lanes[at, :], ghost_wide[...])).astype(BF16)
        pairs[at, :latent] = pairs[at, :latent] + got
        return carry

    lax.fori_loop(0, steps, second_pass, 0)
    take_ghosts(1)

    def third_pass(i, carry):
        at = pl.ds(pl.multiple_of(i * chunk, chunk), chunk)
        got = choose(s_block[at, :], own + FOLDS, mm(s_lanes[at, :], ghost_wide[...])).astype(BF16)
        pairs[at, :latent] = pairs[at, :latent] + got
        pre = mm(pairs[at, :], wei_ref[...])
        s = sigmoid(pre)
        act = (pre * s).astype(BF16)
        act_ref[at, :] = act
        slope_ref[at, :] = slope(s, pre)
        wide_r[at, :] = spread(mm(act, weo_ref[...]).astype(BF16), r_block[at, :])
        return carry

    lax.fori_loop(0, steps, third_pass, 0)

    both[:, :latent] = nodes_ref[...]
    summed = mm(r_rows[...], wide_r[...])
    for j in range(FOLDS):
        both[j * slots : (j + 1) * slots, latent:] = summed[:, j * latent : (j + 1) * latent].astype(BF16)
    node_pre = mm(both[...], wni_ref[...])
    s = sigmoid(node_pre)
    node_act = (node_pre * s).astype(BF16)
    node_slope[...] = slope(s, node_pre)
    fine = (nodes_ref[...].astype(F32) + mm(node_act, wno_ref[...])).astype(BF16)
    fine_ref[...] = fine
    window = mm(pick_sublanes(pool_ref[...], co + 2 * BAND), fine)
    rims[0] = window[: 2 * BAND].astype(BF16)
    rims[1] = window[co:].astype(BF16)
    pool_rims.start()

    dc_rims.wait()
    d_coarse = d_coarse_ref[...]
    d_wide = jnp.concatenate([got_dc[0], d_coarse, got_dc[1]], axis=0)
    d_act = mm_t(d_wide, wco_ref[...])
    pool_hot = pick_lanes(columns(pool_ref[...]), co + 2 * BAND)
    pool_rims.wait()
    coarse_in = (0.125 * jnp.concatenate(
        [
            window[: 2 * BAND] + got_rims[0].astype(F32),
            window[2 * BAND : co],
            window[co:] + got_rims[1].astype(F32),
        ],
        axis=0,
    )).astype(BF16)
    pre = mm(coarse_in, wci_ref[...])
    s = sigmoid(pre)
    d_pre = (d_act * slope(s, pre)).astype(BF16)
    reach = (d_wide.astype(F32) + mm_t(d_pre, wci_ref[...])).astype(BF16)

    d_total = d_fine_ref[...].astype(F32) + 0.125 * mm(pool_hot, reach)
    d16 = d_total.astype(BF16)
    d_node = (mm_t(d16, wno_ref[...]) * node_slope[...]).astype(BF16)
    d_summed = mm_t(d_node, wni_ref[latent:, :]).astype(BF16)
    for j in range(FOLDS):
        ghost_wide[:, j * latent : (j + 1) * latent] = d_summed[j * slots : (j + 1) * slots]
    grad_ref[...] = d_total + mm_t(d_node, wni_ref[:latent, :])
    mid = slice(BAND, co + BAND)
    act = (pre * s)[mid].astype(BF16)
    coarse_ref[...] = (coarse_in[mid].astype(F32) + mm(act, wco_ref[...])).astype(BF16)
    early.load([
        t_mm(both[...], d_node), t_mm(node_act, d16), t_mm(coarse_in[mid], d_pre[mid]), t_mm(act, d_coarse)])
    g_in[...] = jnp.zeros_like(g_in)
    g_out[...] = jnp.zeros_like(g_out)

    def back_pass(i, carry):
        at = pl.ds(pl.multiple_of(i * chunk, chunk), chunk)
        r_blk = r_block[at, :]
        d_message = choose(r_blk, 0, mm(r_lanes[at, :], ghost_wide[...])).astype(BF16)
        g_out[...] += t_mm(act_ref[at, :], d_message)
        d_edge = (mm_t(d_message, weo_ref[...]) * slope_ref[at, :]).astype(BF16)
        g_in[...] += t_mm(pairs[at, :], d_edge)
        wide_r[at, :] = spread(d_edge, r_blk)
        wide_s[at, :] = spread(d_edge, s_block[at, :] & (FOLDS - 1))
        return carry

    lax.fori_loop(0, steps, back_pass, 0)
    late.load([g_in[...], g_out[...]])
    early.across()

    w_send, w_recv = wei_ref[:latent, :], wei_ref[latent:, :]

    def give_ghosts(group):
        sums = mm(s_rows[1 + group], wide_s[...]).astype(BF16)
        for j, k in enumerate(GHOST_ORDER[group * FOLDS : (group + 1) * FOLDS]):
            back_out[k] = mm_t(sums[:, j * latent : (j + 1) * latent], w_send).astype(BF16)
            start(returns, returned, k)

    give_ghosts(1)
    give_ghosts(0)
    late.across()
    early.along()
    sums_s = mm(s_rows[0], wide_s[...]).astype(BF16)
    sums_r = mm(r_rows[...], wide_r[...]).astype(BF16)
    for j in range(FOLDS):
        at = slice(j * slots, (j + 1) * slots)
        lanes = slice(j * latent, (j + 1) * latent)
        grad_ref[at, :] += mm_t(sums_s[:, lanes], w_send) + mm_t(sums_r[:, lanes], w_recv)
    late.along()
    for k in range(peers):
        wait_recv(returns, returned, k)
        wide_s[k * slots : (k + 1) * slots, :] = spread(back[k], ghost_block[k])
    sums_g = mm(g_rows[...], wide_s[: peers * slots, :])
    for j in range(FOLDS):
        grad_ref[j * slots : (j + 1) * slots, :] += sums_g[:, j * latent : (j + 1) * latent]
    early.finish()
    late.finish()
    wait_sends(found, sent)
    wait_sends(returns, returned)
    dc_rims.drain()
    pool_rims.drain()


def final_kernel(
    scale, fine_in, coarse_in, grad_in, early_in, late_in,
    fine_out, coarse_out, grad_out, ei_ref, eo_ref, ni_ref, no_ref, ci_ref, co_ref,
):
    fine_out[...] = fine_in[...]
    coarse_out[...] = coarse_in[...]
    grad_out[...] = grad_in[...]

    def put(total_ref, refs):
        flat = total_ref[...].reshape(-1, total_ref.shape[-1]).astype(F32) * scale
        at = 0
        for ref in refs:
            ref[...] = flat[at : at + ref.shape[0]]
            at += ref.shape[0]

    put(early_in, (ni_ref, no_ref, ci_ref, co_ref))
    put(late_in, (ei_ref, eo_ref))


def body(
    n_gx, n_gy, nodes, ghost_rows, ghost_count, edge_send, edge_recv, edge_count, pool_map,
    w_edge_in, w_edge_out, w_node_in, w_node_out, w_coarse_in, w_coarse_out, d_fine, d_coarse,
):
    rows, latent = nodes.shape
    _, peers, slots = ghost_rows.shape
    edges_n = edge_send.shape[1]
    co = d_coarse.shape[0]
    chunk = 2048 if edges_n % 2048 == 0 else edges_n
    groups = (rows // slots + peers) // FOLDS
    dma = pltpu.SemaphoreType.DMA
    vmem = pl.BlockSpec(memory_space=pltpu.VMEM)
    smem = pl.BlockSpec(memory_space=pltpu.SMEM)
    early_rows, late_rows = 5 * latent // n_gx, 3 * latent // n_gx

    def total_buffers(share):
        return [
            pltpu.VMEM((n_gx, share, latent), BF16), pltpu.VMEM((n_gx - 1, share, latent), BF16),
            pltpu.VMEM((n_gy, share, latent), BF16), pltpu.VMEM((share, latent), BF16)]

    total_sems = [dma((n_gx - 1,))] * 2 + [dma((n_gy - 1,))] * 2 + [dma((n_gx - 1,))] * 2
    halo = pltpu.VMEM((peers, slots, latent), BF16)
    arrays = (nodes, ghost_rows, ghost_count, edge_send, edge_recv, pool_map, w_edge_in, w_edge_out,
              w_node_in, w_node_out, w_coarse_in, w_coarse_out, d_fine, d_coarse)
    results = pl.pallas_call(
        functools.partial(main_kernel, n_gx, n_gy, chunk),
        out_shape=[
            jax.ShapeDtypeStruct((rows, latent), BF16), jax.ShapeDtypeStruct((co, latent), BF16),
            jax.ShapeDtypeStruct((rows, latent), F32),
            jax.ShapeDtypeStruct((n_gx, early_rows, latent), BF16),
            jax.ShapeDtypeStruct((n_gx, late_rows, latent), BF16)],
        in_specs=[smem] + [pl.BlockSpec(memory_space=pltpu.HBM)] * len(arrays),
        out_specs=[vmem] * 5,
        scratch_shapes=[pltpu.VMEM(x.shape, x.dtype) for x in arrays] + [dma((len(arrays),))] + [halo] * 4 + [
            pltpu.VMEM((slots, FOLDS * latent), BF16), pltpu.VMEM((slots, FOLDS * latent), BF16),
            pltpu.VMEM((peers, slots, LANES), jnp.int32),
            pltpu.VMEM((1, edges_n), jnp.int32), pltpu.VMEM((1, edges_n), jnp.int32),
            pltpu.VMEM((edges_n, LANES), jnp.int32), pltpu.VMEM((edges_n, LANES), jnp.int32),
            pltpu.VMEM((edges_n, slots), BF16), pltpu.VMEM((edges_n, slots), BF16),
            pltpu.VMEM((slots, edges_n), BF16), pltpu.VMEM((groups, slots, edges_n), BF16),
            pltpu.VMEM((slots, peers * slots), BF16),
            pltpu.VMEM((edges_n, 2 * latent), BF16), pltpu.VMEM((edges_n, latent), BF16),
            pltpu.VMEM((edges_n, latent), F32),
            pltpu.VMEM((edges_n, FOLDS * latent), BF16), pltpu.VMEM((edges_n, FOLDS * latent), BF16),
            pltpu.VMEM((rows, 2 * latent), BF16), pltpu.VMEM((rows, latent), F32),
            pltpu.VMEM((2, 2 * BAND, latent), BF16), pltpu.VMEM((2, 2 * BAND, latent), BF16),
            pltpu.VMEM((2, BAND, latent), BF16),
            pltpu.VMEM((2 * latent, latent), F32), pltpu.VMEM((latent, latent), F32),
        ] + total_buffers(early_rows) + total_buffers(late_rows)
        + [dma((peers,))] * 4 + [dma((2, 2))] * 2 + total_sems * 2,
        compiler_params=pltpu.CompilerParams(
            vmem_limit_bytes=48 * 1024 * 1024, collective_id=0, has_side_effects=True),
    )(edge_count, *(pltpu.with_memory_space_constraint(x, pltpu.HBM) for x in arrays))
    scale = 1.0 / (rows * n_gx * n_gy) ** 0.5
    fine, coarse, grads, ei, eo, ni, no, ci, co_grad = pl.pallas_call(
        functools.partial(final_kernel, scale),
        out_shape=[
            jax.ShapeDtypeStruct((rows, latent), BF16), jax.ShapeDtypeStruct((co, latent), BF16),
            jax.ShapeDtypeStruct((rows, latent), F32)] + [
            jax.ShapeDtypeStruct((n * latent, latent), F32) for n in (2, 1, 2, 1, 1, 1)],
        in_specs=[vmem] * 5,
        out_specs=[vmem] * 9,
        compiler_params=pltpu.CompilerParams(vmem_limit_bytes=8 * 1024 * 1024),
    )(*results)
    return fine, coarse, grads, ei, eo, ni, no, ci, co_grad


def solution(mesh):
    split = P(("gx", "gy"), None)
    return jax.shard_map(
        functools.partial(body, mesh.shape["gx"], mesh.shape["gy"]),
        mesh=mesh,
        in_specs=(split, P(("gx", "gy"), None, None), split, split, split, P(("gx", "gy")), split)
        + (P(),) * 6
        + (split, split),
        out_specs=(split, split, split) + (P(),) * 6,
        check_vma=False,
    )
```

```python
import functools

import jax
import jax.numpy as jnp
from jax import lax
from jax.experimental import pallas as pl
from jax.experimental.pallas import tpu as pltpu
from jax.sharding import PartitionSpec as P

BAND = 32
MESH = pl.DeviceIdType.MESH
ACROSS = (-1, -1, -1, 0, 0, 1, 1, 1)
ALONG = (-1, 0, 1, -1, 1, -1, 0, 1)
SEND_ORDER = (3, 4, 1, 6, 0, 2, 5, 7)
GHOST_ORDER = (1, 6, 3, 4, 0, 2, 5, 7)
F32 = jnp.float32
BF16 = jnp.bfloat16
FOLDS = 4
NOWHERE = 32767
LANES = 128


def mm(a, b):
    return jnp.dot(a, b, preferred_element_type=F32)


def mm_t(a, b):
    return lax.dot_general(a, b, (((1,), (1,)), ((), ())), preferred_element_type=F32)


def t_mm(a, b):
    return lax.dot_general(a, b, (((0,), (0,)), ((), ())), preferred_element_type=F32)


def sigmoid(v):
    return 0.5 * jnp.tanh(0.5 * v) + 0.5


def columns(row):
    return jnp.concatenate(
        [
            jnp.transpose(jnp.broadcast_to(row[:, s : s + LANES], (LANES, LANES)))
            for s in range(0, row.shape[1], LANES)
        ],
        axis=0,
    )


def alive(row, start, count):
    ids = lax.broadcasted_iota(jnp.int32, row.shape, 1) + start
    return jnp.where(ids < count, row, -1)


def hot(ids, index):
    return jnp.where(ids == index, jnp.ones((), BF16), jnp.zeros((), BF16))


def pick_lanes(col, first, width):
    ids = lax.broadcasted_iota(jnp.int16, (col.shape[0], LANES), 1)
    parts = [
        hot(ids + jnp.int16(first + s), col)[:, : min(LANES, width - s)] for s in range(0, width, LANES)
    ]
    return jnp.concatenate(parts, axis=1)


def pick_sublanes(row, height):
    return hot(lax.broadcasted_iota(jnp.int16, (height, row.shape[1]), 0), row.astype(jnp.int16))


def choose(fold, wide):
    width = wide.shape[1] // FOLDS
    out = wide[:, :width]
    for j in range(1, FOLDS):
        out = jnp.where(fold == j, wide[:, j * width : (j + 1) * width], out)
    return out


def spread(values, fold):
    return jnp.concatenate(
        [jnp.where(fold == jnp.int16(j), values, jnp.zeros((), BF16)) for j in range(FOLDS)], axis=1
    )


def piece(sums, j):
    width = sums.shape[1] // FOLDS
    return sums[:, j * width : (j + 1) * width]


def slope(s, v):
    return s * (1.0 + v * (1.0 - s))


def neighbours(n_gx, n_gy, sign):
    a, b = lax.axis_index("gx"), lax.axis_index("gy")
    found = []
    for dx, dy in zip(ACROSS, ALONG):
        dx, dy = sign * dx, sign * dy
        ta, tb = a + dx, b + dy
        sa, sb = a - dx, b - dy
        there = (ta >= 0) & (ta < n_gx) & (tb >= 0) & (tb < n_gy)
        here = (sa >= 0) & (sa < n_gx) & (sb >= 0) & (sb < n_gy)
        target = (jnp.clip(ta, 0, n_gx - 1), jnp.clip(tb, 0, n_gy - 1))
        found.append((target, there, here))
    return found


def remote(src, dst, send, recv, peer):
    return pltpu.make_async_remote_copy(
        src_ref=src, dst_ref=dst, send_sem=send, recv_sem=recv, device_id=peer, device_id_type=MESH)


def exchange_copies(found, src_ref, dst_ref, send_sem, recv_sem):
    return [
        remote(src_ref.at[k], dst_ref.at[k], send_sem.at[k], recv_sem.at[k], found[k][0])
        for k in range(len(found))
    ]


def clear_absent(found, dst_ref):
    for k in range(len(found)):
        @pl.when(jnp.logical_not(found[k][2]))
        def _(k=k):
            dst_ref[k] = jnp.zeros(dst_ref.shape[1:], dst_ref.dtype)


def start(found, copies, k):
    @pl.when(found[k][1])
    def _():
        copies[k].start()


def wait_recv(found, copies, k):
    @pl.when(found[k][2])
    def _():
        copies[k].wait_recv()


def wait_sends(found, copies):
    for k in range(len(found)):
        @pl.when(found[k][1])
        def _(k=k):
            copies[k].wait_send()


class Rims:
    def __init__(self, n_gy, low, high, got, send_sem, recv_sem):
        a, b = lax.axis_index("gx"), lax.axis_index("gy")
        self.below, self.above = b > 0, b < n_gy - 1
        self.down = remote(low, got.at[1], send_sem.at[0], recv_sem.at[1], (a, jnp.maximum(b - 1, 0)))
        self.up = remote(high, got.at[0], send_sem.at[1], recv_sem.at[0], (a, jnp.minimum(b + 1, n_gy - 1)))
        self.got = got

    def start(self):
        @pl.when(self.below)
        def _():
            self.down.start()

        @pl.when(self.above)
        def _():
            self.up.start()

        for slot, there in ((0, self.below), (1, self.above)):
            @pl.when(jnp.logical_not(there))
            def _(slot=slot):
                self.got[slot] = jnp.zeros(self.got.shape[1:], self.got.dtype)

    def wait(self):
        @pl.when(self.below)
        def _():
            self.up.wait_recv()

        @pl.when(self.above)
        def _():
            self.down.wait_recv()

    def drain(self):
        @pl.when(self.below)
        def _():
            self.down.wait_send()

        @pl.when(self.above)
        def _():
            self.up.wait_send()


class Total:
    def __init__(self, peers_x, peers_y, total, g16, got_x, got_y, mine, xs, xr, ys, yr, zs, zr):
        a, b = lax.axis_index("gx"), lax.axis_index("gy")
        self.n_gy = len(peers_y) + 1
        self.total, self.g16, self.got_x, self.got_y, self.mine = total, g16, got_x, got_y, mine
        self.first = [remote(g16.at[p[0]], got_x.at[r], xs.at[r], xr.at[r], p) for r, p in enumerate(peers_x)]
        self.second = [
            remote(got_y.at[0], got_y.at[r + 1], ys.at[r], yr.at[r], p) for r, p in enumerate(peers_y)
        ]
        self.third = [remote(mine, total.at[a], zs.at[r], zr.at[r], p) for r, p in enumerate(peers_x)]

    def load(self, parts):
        flat = jnp.concatenate(parts, axis=0).astype(BF16)
        share = self.g16.shape[1]
        for i in range(self.g16.shape[0]):
            self.g16[i] = flat[i * share : (i + 1) * share]
        for copy in self.first:
            copy.start()

    def across(self):
        acc = self.g16[lax.axis_index("gx")].astype(F32)
        for r, copy in enumerate(self.first):
            copy.wait_recv()
            acc = acc + self.got_x[r].astype(F32)
        self.got_y[0] = acc.astype(BF16)
        for copy in self.second:
            copy.start()

    def along(self):
        a, b = lax.axis_index("gx"), lax.axis_index("gy")
        for copy in self.second:
            copy.wait_recv()
        acc = jnp.zeros(self.mine.shape, F32)
        for y in range(self.n_gy):
            acc = acc + self.got_y[lax.rem(b - y + self.n_gy, self.n_gy)].astype(F32)
        self.mine[...] = acc.astype(BF16)
        for copy in self.third:
            copy.start()
        self.total[a] = acc.astype(BF16)

    def finish(self):
        for copy in self.third:
            copy.wait_recv()
        for copy in self.first + self.second + self.third:
            copy.wait_send()


def main_kernel(
    n_gx, n_gy, chunk,
    ecount_in, nodes_in, rows_in, gcount_in, send_in, recv_in, pool_in,
    wei_in, weo_in, wni_in, wno_in, wci_in, wco_in, d_fine_in, d_coarse_in,
    fine_ref, coarse_ref, grad_ref, early_ref, late_ref,
    ecount_ref, nodes_ref, rows_ref, gcount_ref, send_ref, recv_ref, pool_ref,
    wei_ref, weo_ref, wni_ref, wno_ref, wci_ref, wco_ref, d_fine_ref, d_coarse_ref, load_sem,
    outgoing, arrived, back_out, back, nodes_wide, ghost_wide, ghost_fold,
    srow, rrow, s_fold, r_fold, s_fold16, r_fold16, s_lanes, r_lanes,
    pairs, edge16, slope_ref, wide_r, wide_s, both, agg, node_slope, d_node_ref,
    rims, got_rims, got_dc, g_in,
    e16, e_x, e_y, e_mine, l16, l_x, l_y, l_mine,
    out_s, out_r, ret_s, ret_r, rim_s, rim_r,
    exs, exr, eys, eyr, ezs, ezr, lxs, lxr, lys, lyr, lzs, lzr,
):
    rows, latent = nodes_ref.shape
    edges_n = send_ref.shape[1]
    peers, slots = rows_ref.shape[1:]
    co = d_coarse_ref.shape[0]
    bits = slots.bit_length() - 1
    own = rows // slots
    a, b = lax.axis_index("gx"), lax.axis_index("gy")
    found = neighbours(n_gx, n_gy, 1)
    returns = neighbours(n_gx, n_gy, -1)
    peers_x = [(lax.rem(a + r, n_gx), b) for r in range(1, n_gx)]
    peers_y = [(a, lax.rem(b + r, n_gy)) for r in range(1, n_gy)]
    corners = [f for f, dx, dy in zip(found, ACROSS, ALONG) if dx and dy]

    loads = [
        pltpu.make_async_copy(src, dst, load_sem.at[i])
        for i, (src, dst) in enumerate((
            (rows_in, rows_ref), (gcount_in, gcount_ref), (nodes_in, nodes_ref), (d_coarse_in, d_coarse_ref),
            (send_in, send_ref), (recv_in, recv_ref), (ecount_in, ecount_ref), (wei_in, wei_ref), (weo_in, weo_ref), (wni_in, wni_ref),
            (wno_in, wno_ref), (pool_in, pool_ref), (wco_in, wco_ref), (wci_in, wci_ref), (d_fine_in, d_fine_ref)))
    ]
    for load in loads:
        load.start()
    barrier = pltpu.get_barrier_semaphore()
    expect = jnp.int32(n_gx + n_gy - 2)
    for target, there, _ in corners:
        @pl.when(there)
        def _(target=target):
            pl.semaphore_signal(barrier, inc=1, device_id=target, device_id_type=MESH)
        expect = expect + jnp.where(there, 1, 0)
    for peer in peers_x + peers_y:
        pl.semaphore_signal(barrier, inc=1, device_id=peer, device_id_type=MESH)

    sent = exchange_copies(found, outgoing, arrived, out_s, out_r)
    returned = exchange_copies(returns, back_out, back, ret_s, ret_r)
    dc_rims = Rims(n_gy, d_coarse_ref.at[:BAND], d_coarse_ref.at[co - BAND :], got_dc, rim_s.at[0], rim_r.at[0])
    pool_rims = Rims(n_gy, rims.at[0], rims.at[1], got_rims, rim_s.at[1], rim_r.at[1])
    early = Total(peers_x, peers_y, early_ref, e16, e_x, e_y, e_mine, exs, exr, eys, eyr, ezs, ezr)
    late = Total(peers_x, peers_y, late_ref, l16, l_x, l_y, l_mine, lxs, lxr, lys, lyr, lzs, lzr)

    def code(index):
        fold = (index >> bits) & (FOLDS - 1)
        group = jnp.where(index < 0, NOWHERE, (index >> bits) // FOLDS * slots + (index & (slots - 1)))
        return (fold << 16) | group

    def decode(row):
        col = columns(row)
        fold = col >> 16
        return col.astype(jnp.int16), fold, fold.astype(jnp.int16)

    def place(index, group):
        mine = (index >= group * FOLDS * slots) & (index < (group + 1) * FOLDS * slots)
        return jnp.where(mine, index & (slots - 1), -1)

    def ghost_row(k):
        return alive(rows_ref[0, k : k + 1, :], 0, gcount_ref[:, k : k + 1])

    for load in loads[:3]:
        load.wait()
    for j in range(own):
        nodes_wide[:, j * latent : (j + 1) * latent] = nodes_ref[j * slots : (j + 1) * slots]
    for at in range(0, peers, FOLDS):
        batch = SEND_ORDER[at : at + FOLDS]
        where, fold, fold16 = decode(jnp.concatenate([code(ghost_row(k)) for k in batch], axis=1))
        picked = choose(fold, mm(pick_lanes(where, 0, slots), nodes_wide[...])).astype(BF16)
        for n, k in enumerate(batch):
            ghost_fold[k] = fold16[n * slots : (n + 1) * slots]
            outgoing[k] = picked[n * slots : (n + 1) * slots]
        if at == 0:
            pl.semaphore_wait(barrier, expect)
        for k in batch:
            start(found, sent, k)
    for load in loads[3:]:
        load.wait()
    dc_rims.start()
    clear_absent(found, arrived)
    clear_absent(returns, back)

    send = send_ref[...]
    moved = send
    for p, k in enumerate(GHOST_ORDER):
        moved = jnp.where((send >> bits) == own + k, (send & (slots - 1)) + ((own + p) << bits), moved)
    srow[...] = moved
    rrow[...] = alive(recv_ref[...], 0, ecount_ref[0])

    def first_pass(i, carry):
        at = pl.ds(pl.multiple_of(i * chunk, chunk), chunk)
        s_where, s_f, s_fold16[at, :] = decode(code(srow[:, at]))
        r_where, r_f, r_fold16[at, :] = decode(code(rrow[:, at]))
        s_fold[at, :] = s_f
        r_fold[at, :] = r_f
        for t in range(s_lanes.shape[0]):
            s_lanes[t, at, :] = pick_lanes(s_where, t * slots, slots)
        r_lanes[at, :] = pick_lanes(r_where, 0, slots)
        pairs[at, :latent] = choose(s_f, mm(s_lanes[0, at, :], nodes_wide[...])).astype(BF16)
        pairs[at, latent:] = choose(r_f, mm(r_lanes[at, :], nodes_wide[...])).astype(BF16)
        return carry

    steps = edges_n // chunk
    lax.fori_loop(0, steps, first_pass, 0)

    def take_ghosts(group):
        for j, k in enumerate(GHOST_ORDER[group * FOLDS : (group + 1) * FOLDS]):
            wait_recv(found, sent, k)
        for j, k in enumerate(GHOST_ORDER[group * FOLDS : (group + 1) * FOLDS]):
            ghost_wide[:, j * latent : (j + 1) * latent] = arrived[k]

    take_ghosts(0)

    def second_pass(i, carry):
        at = pl.ds(pl.multiple_of(i * chunk, chunk), chunk)
        got = choose(s_fold[at, :], mm(s_lanes[1, at, :], ghost_wide[...])).astype(BF16)
        pairs[at, :latent] = pairs[at, :latent] + got
        return carry

    lax.fori_loop(0, steps, second_pass, 0)
    take_ghosts(1)

    def third_pass(i, carry):
        at = pl.ds(pl.multiple_of(i * chunk, chunk), chunk)
        got = choose(s_fold[at, :], mm(s_lanes[2, at, :], ghost_wide[...])).astype(BF16)
        pairs[at, :latent] = pairs[at, :latent] + got
        pre = mm(pairs[at, :], wei_ref[...])
        s = sigmoid(pre)
        act = pre * s
        slope_ref[at, :] = s + act * (1.0 - s)
        wide_r[at, :] = spread(act.astype(BF16), r_fold16[at, :])
        return carry

    lax.fori_loop(0, steps, third_pass, 0)

    both[:, :latent] = nodes_ref[...]
    acts = mm(pick_sublanes(place(rrow[...], 0), slots), wide_r[...]).astype(BF16)
    for j in range(FOLDS):
        agg[j * slots : (j + 1) * slots, :] = piece(acts, j)
    both[:, latent:] = mm(agg[...], weo_ref[...]).astype(BF16)
    node_pre = mm(both[...], wni_ref[...])
    s = sigmoid(node_pre)
    node_act = (node_pre * s).astype(BF16)
    node_slope[...] = slope(s, node_pre)
    fine = (nodes_ref[...].astype(F32) + mm(node_act, wno_ref[...])).astype(BF16)
    fine_ref[...] = fine
    window = mm(pick_sublanes(pool_ref[...], co + 2 * BAND), fine)
    rims[0] = window[: 2 * BAND].astype(BF16)
    rims[1] = window[co:].astype(BF16)
    pool_rims.start()

    dc_rims.wait()
    d_coarse = d_coarse_ref[...]
    d_wide = jnp.concatenate([got_dc[0], d_coarse, got_dc[1]], axis=0)
    d_act = mm_t(d_wide, wco_ref[...])
    pool_hot = pick_lanes(columns(pool_ref[...]).astype(jnp.int16), 0, co + 2 * BAND)
    pool_rims.wait()
    coarse_in = (0.125 * jnp.concatenate(
        [
            window[: 2 * BAND] + got_rims[0].astype(F32),
            window[2 * BAND : co],
            window[co:] + got_rims[1].astype(F32),
        ],
        axis=0,
    )).astype(BF16)
    pre = mm(coarse_in, wci_ref[...])
    s = sigmoid(pre)
    d_pre = (d_act * slope(s, pre)).astype(BF16)
    reach = (d_wide.astype(F32) + mm_t(d_pre, wci_ref[...])).astype(BF16)

    d_total = d_fine_ref[...].astype(F32) + 0.125 * mm(pool_hot, reach)
    d16 = d_total.astype(BF16)
    d_node = (mm_t(d16, wno_ref[...]) * node_slope[...]).astype(BF16)
    d_summed = mm_t(d_node, wni_ref[latent:, :]).astype(BF16)
    d_edge_out = mm_t(d_summed, weo_ref[...]).astype(BF16)
    for j in range(FOLDS):
        ghost_wide[:, j * latent : (j + 1) * latent] = d_edge_out[j * slots : (j + 1) * slots]
    d_node_ref[...] = d_node
    grad_ref[...] = d_total
    mid = slice(BAND, co + BAND)
    act = (pre * s)[mid].astype(BF16)
    coarse_ref[...] = (coarse_in[mid].astype(F32) + mm(act, wco_ref[...])).astype(BF16)
    early.load([
        t_mm(both[...], d_node), t_mm(node_act, d16), t_mm(coarse_in[mid], d_pre[mid]), t_mm(act, d_coarse),
        t_mm(agg[...], d_summed)])
    g_in[...] = jnp.zeros_like(g_in)

    def back_pass(i, carry):
        at = pl.ds(pl.multiple_of(i * chunk, chunk), chunk)
        d_act = choose(r_fold[at, :], mm(r_lanes[at, :], ghost_wide[...]))
        d_edge = (d_act * slope_ref[at, :]).astype(BF16)
        edge16[at, :] = d_edge
        g_in[...] += t_mm(pairs[at, :], d_edge)
        return carry

    lax.fori_loop(0, steps, back_pass, 0)
    late.load([g_in[...]])
    w_send, w_recv = wei_ref[:latent, :], wei_ref[latent:, :]
    wide_s[...] = spread(edge16[...], s_fold16[...])

    def send_sums(group):
        return mm(pick_sublanes(place(srow[...], group), slots), wide_s[...]).astype(BF16)

    def give_ghosts(group):
        sums = send_sums(1 + group)
        for j, k in enumerate(GHOST_ORDER[group * FOLDS : (group + 1) * FOLDS]):
            back_out[k] = mm_t(piece(sums, j), w_send).astype(BF16)
        for k in GHOST_ORDER[group * FOLDS : (group + 1) * FOLDS]:
            start(returns, returned, k)

    give_ghosts(0)
    wide_r[...] = spread(edge16[...], r_fold16[...])
    sums_r = mm(pick_sublanes(place(rrow[...], 0), slots), wide_r[...]).astype(BF16)
    for j in range(FOLDS):
        grad_ref[j * slots : (j + 1) * slots, :] += mm_t(piece(sums_r, j), w_recv)
    early.across()
    late.across()
    give_ghosts(1)
    sums_s = send_sums(0)
    for j in range(FOLDS):
        grad_ref[j * slots : (j + 1) * slots, :] += mm_t(piece(sums_s, j), w_send)
    grad_ref[...] += mm_t(d_node_ref[...], wni_ref[:latent, :])
    early.along()
    late.along()
    for k in range(peers):
        wait_recv(returns, returned, k)
        wide_s[k * slots : (k + 1) * slots, :] = spread(back[k], ghost_fold[k])
    ghosts = jnp.concatenate([place(ghost_row(k), 0) for k in range(peers)], axis=1)
    sums_g = mm(pick_sublanes(ghosts, slots), wide_s[: peers * slots, :])
    for j in range(FOLDS):
        grad_ref[j * slots : (j + 1) * slots, :] += piece(sums_g, j)
    early.finish()
    late.finish()
    wait_sends(found, sent)
    wait_sends(returns, returned)
    dc_rims.drain()
    pool_rims.drain()


def final_kernel(
    scale, fine_in, coarse_in, grad_in, early_in, late_in,
    fine_out, coarse_out, grad_out, ei_ref, eo_ref, ni_ref, no_ref, ci_ref, co_ref,
):
    fine_out[...] = fine_in[...]
    coarse_out[...] = coarse_in[...]
    grad_out[...] = grad_in[...]

    def put(total_ref, refs):
        flat = total_ref[...].reshape(-1, total_ref.shape[-1]).astype(F32) * scale
        at = 0
        for ref in refs:
            ref[...] = flat[at : at + ref.shape[0]]
            at += ref.shape[0]

    put(early_in, (ni_ref, no_ref, ci_ref, co_ref, eo_ref))
    put(late_in, (ei_ref,))


def body(
    n_gx, n_gy, nodes, ghost_rows, ghost_count, edge_send, edge_recv, edge_count, pool_map,
    w_edge_in, w_edge_out, w_node_in, w_node_out, w_coarse_in, w_coarse_out, d_fine, d_coarse,
):
    rows, latent = nodes.shape
    _, peers, slots = ghost_rows.shape
    edges_n = edge_send.shape[1]
    co = d_coarse.shape[0]
    chunk = edges_n
    groups = (rows // slots + peers) // FOLDS
    dma = pltpu.SemaphoreType.DMA
    vmem = pl.BlockSpec(memory_space=pltpu.VMEM)
    hbm = pl.BlockSpec(memory_space=pltpu.HBM)
    early_rows, late_rows = 6 * latent // n_gx, 2 * latent // n_gx

    def total_buffers(share):
        return [
            pltpu.VMEM((n_gx, share, latent), BF16), pltpu.VMEM((n_gx - 1, share, latent), BF16),
            pltpu.VMEM((n_gy, share, latent), BF16), pltpu.VMEM((share, latent), BF16)]

    total_sems = [dma((n_gx - 1,))] * 2 + [dma((n_gy - 1,))] * 2 + [dma((n_gx - 1,))] * 2
    halo = pltpu.VMEM((peers, slots, latent), BF16)
    arrays = (edge_count, nodes, ghost_rows, ghost_count, edge_send, edge_recv, pool_map, w_edge_in, w_edge_out,
              w_node_in, w_node_out, w_coarse_in, w_coarse_out, d_fine, d_coarse)
    results = pl.pallas_call(
        functools.partial(main_kernel, n_gx, n_gy, chunk),
        out_shape=[
            jax.ShapeDtypeStruct((rows, latent), BF16), jax.ShapeDtypeStruct((co, latent), BF16),
            jax.ShapeDtypeStruct((rows, latent), F32),
            jax.ShapeDtypeStruct((n_gx, early_rows, latent), BF16),
            jax.ShapeDtypeStruct((n_gx, late_rows, latent), BF16)],
        in_specs=[pl.BlockSpec(memory_space=pl.ANY)] + [hbm] * (len(arrays) - 1),
        out_specs=[vmem] * 5,
        scratch_shapes=[pltpu.SMEM((1,), jnp.int32)] + [pltpu.VMEM(x.shape, x.dtype) for x in arrays[1:]] + [dma((len(arrays),))] + [halo] * 4 + [
            pltpu.VMEM((slots, FOLDS * latent), BF16), pltpu.VMEM((slots, FOLDS * latent), BF16),
            pltpu.VMEM((peers, slots, LANES), jnp.int16),
            pltpu.VMEM((1, edges_n), jnp.int32), pltpu.VMEM((1, edges_n), jnp.int32),
            pltpu.VMEM((edges_n, LANES), jnp.int32), pltpu.VMEM((edges_n, LANES), jnp.int32),
            pltpu.VMEM((edges_n, LANES), jnp.int16), pltpu.VMEM((edges_n, LANES), jnp.int16),
            pltpu.VMEM((groups, edges_n, slots), BF16), pltpu.VMEM((edges_n, slots), BF16),
            pltpu.VMEM((edges_n, 2 * latent), BF16), pltpu.VMEM((edges_n, latent), BF16),
            pltpu.VMEM((edges_n, latent), F32),
            pltpu.VMEM((edges_n, FOLDS * latent), BF16), pltpu.VMEM((edges_n, FOLDS * latent), BF16),
            pltpu.VMEM((rows, 2 * latent), BF16), pltpu.VMEM((rows, latent), BF16),
            pltpu.VMEM((rows, latent), F32), pltpu.VMEM((rows, latent), BF16),
            pltpu.VMEM((2, 2 * BAND, latent), BF16), pltpu.VMEM((2, 2 * BAND, latent), BF16),
            pltpu.VMEM((2, BAND, latent), BF16),
            pltpu.VMEM((2 * latent, latent), F32),
        ] + total_buffers(early_rows) + total_buffers(late_rows)
        + [dma((peers,))] * 4 + [dma((2, 2))] * 2 + total_sems * 2,
        compiler_params=pltpu.CompilerParams(
            vmem_limit_bytes=48 * 1024 * 1024, collective_id=0, has_side_effects=True),
    )(edge_count, *(pltpu.with_memory_space_constraint(x, pltpu.HBM) for x in arrays[1:]))
    scale = 1.0 / (rows * n_gx * n_gy) ** 0.5
    fine, coarse, grads, ei, eo, ni, no, ci, co_grad = pl.pallas_call(
        functools.partial(final_kernel, scale),
        out_shape=[
            jax.ShapeDtypeStruct((rows, latent), BF16), jax.ShapeDtypeStruct((co, latent), BF16),
            jax.ShapeDtypeStruct((rows, latent), F32)] + [
            jax.ShapeDtypeStruct((n * latent, latent), F32) for n in (2, 1, 2, 1, 1, 1)],
        in_specs=[vmem] * 5,
        out_specs=[vmem] * 9,
        compiler_params=pltpu.CompilerParams(vmem_limit_bytes=8 * 1024 * 1024),
    )(*results)
    return fine, coarse, grads, ei, eo, ni, no, ci, co_grad


def solution(mesh):
    split = P(("gx", "gy"), None)
    return jax.shard_map(
        functools.partial(body, mesh.shape["gx"], mesh.shape["gy"]),
        mesh=mesh,
        in_specs=(split, P(("gx", "gy"), None, None), split, split, split, P(("gx", "gy")), split)
        + (P(),) * 6
        + (split, split),
        out_specs=(split, split, split) + (P(),) * 6,
        check_vma=False,
    )
```

```python
import functools

import jax
import jax.numpy as jnp
from jax import lax
from jax.experimental import pallas as pl
from jax.experimental.pallas import tpu as pltpu
from jax.sharding import PartitionSpec as P

BAND = 32
MESH = pl.DeviceIdType.MESH
ACROSS = (-1, -1, -1, 0, 0, 1, 1, 1)
ALONG = (-1, 0, 1, -1, 1, -1, 0, 1)
SEND_ORDER = (3, 4, 1, 6, 0, 2, 5, 7)
GHOST_ORDER = (1, 6, 3, 4, 0, 2, 5, 7)
F32 = jnp.float32
BF16 = jnp.bfloat16
FOLDS = 4
NOWHERE = 32767
LANES = 128


def mm(a, b):
    return jnp.dot(a, b, preferred_element_type=F32)


def mm_t(a, b):
    return lax.dot_general(a, b, (((1,), (1,)), ((), ())), preferred_element_type=F32)


def t_mm(a, b):
    return lax.dot_general(a, b, (((0,), (0,)), ((), ())), preferred_element_type=F32)


def sigmoid(v):
    return 0.5 * jnp.tanh(0.5 * v) + 0.5


def columns(row):
    return jnp.concatenate(
        [
            jnp.transpose(jnp.broadcast_to(row[:, s : s + LANES], (LANES, LANES)))
            for s in range(0, row.shape[1], LANES)
        ],
        axis=0,
    )


def alive(row, start, count):
    ids = lax.broadcasted_iota(jnp.int32, row.shape, 1) + start
    return jnp.where(ids < count, row, -1)


def hot(ids, index):
    return jnp.where(ids == index, jnp.ones((), BF16), jnp.zeros((), BF16))


def pick_lanes(col, first, width):
    ids = lax.broadcasted_iota(jnp.int16, (col.shape[0], LANES), 1)
    parts = [
        hot(ids + jnp.int16(first + s), col)[:, : min(LANES, width - s)] for s in range(0, width, LANES)
    ]
    return jnp.concatenate(parts, axis=1)


def pick_sublanes(row, height):
    return hot(lax.broadcasted_iota(jnp.int16, (height, row.shape[1]), 0), row.astype(jnp.int16))


def choose(fold, wide):
    width = wide.shape[1] // FOLDS
    out = wide[:, :width]
    for j in range(1, FOLDS):
        out = jnp.where(fold == j, wide[:, j * width : (j + 1) * width], out)
    return out


def spread(values, fold):
    return jnp.concatenate(
        [jnp.where(fold == jnp.int16(j), values, jnp.zeros((), BF16)) for j in range(FOLDS)], axis=1
    )


def piece(sums, j):
    width = sums.shape[1] // FOLDS
    return sums[:, j * width : (j + 1) * width]


def slope(s, v):
    return s * (1.0 + v * (1.0 - s))


def neighbours(n_gx, n_gy, sign):
    a, b = lax.axis_index("gx"), lax.axis_index("gy")
    found = []
    for dx, dy in zip(ACROSS, ALONG):
        dx, dy = sign * dx, sign * dy
        ta, tb = a + dx, b + dy
        sa, sb = a - dx, b - dy
        there = (ta >= 0) & (ta < n_gx) & (tb >= 0) & (tb < n_gy)
        here = (sa >= 0) & (sa < n_gx) & (sb >= 0) & (sb < n_gy)
        target = (jnp.clip(ta, 0, n_gx - 1), jnp.clip(tb, 0, n_gy - 1))
        found.append((target, there, here))
    return found


def remote(src, dst, send, recv, peer):
    return pltpu.make_async_remote_copy(
        src_ref=src, dst_ref=dst, send_sem=send, recv_sem=recv, device_id=peer, device_id_type=MESH)


def exchange_copies(found, src_ref, dst_ref, send_sem, recv_sem):
    return [
        remote(src_ref.at[k], dst_ref.at[k], send_sem.at[k], recv_sem.at[k], found[k][0])
        for k in range(len(found))
    ]


def clear_absent(found, dst_ref):
    for k in range(len(found)):
        @pl.when(jnp.logical_not(found[k][2]))
        def _(k=k):
            dst_ref[k] = jnp.zeros(dst_ref.shape[1:], dst_ref.dtype)


def start(found, copies, k):
    @pl.when(found[k][1])
    def _():
        copies[k].start()


def wait_recv(found, copies, k):
    @pl.when(found[k][2])
    def _():
        copies[k].wait_recv()


def wait_sends(found, copies):
    for k in range(len(found)):
        @pl.when(found[k][1])
        def _(k=k):
            copies[k].wait_send()


class Rims:
    def __init__(self, n_gy, low, high, got, send_sem, recv_sem):
        a, b = lax.axis_index("gx"), lax.axis_index("gy")
        self.below, self.above = b > 0, b < n_gy - 1
        self.down = remote(low, got.at[1], send_sem.at[0], recv_sem.at[1], (a, jnp.maximum(b - 1, 0)))
        self.up = remote(high, got.at[0], send_sem.at[1], recv_sem.at[0], (a, jnp.minimum(b + 1, n_gy - 1)))
        self.got = got

    def start(self):
        @pl.when(self.below)
        def _():
            self.down.start()

        @pl.when(self.above)
        def _():
            self.up.start()

        for slot, there in ((0, self.below), (1, self.above)):
            @pl.when(jnp.logical_not(there))
            def _(slot=slot):
                self.got[slot] = jnp.zeros(self.got.shape[1:], self.got.dtype)

    def wait(self):
        @pl.when(self.below)
        def _():
            self.up.wait_recv()

        @pl.when(self.above)
        def _():
            self.down.wait_recv()

    def drain(self):
        @pl.when(self.below)
        def _():
            self.down.wait_send()

        @pl.when(self.above)
        def _():
            self.up.wait_send()


class Total:
    def __init__(self, peers_x, peers_y, total, g16, got_x, got_y, mine, xs, xr, ys, yr, zs, zr):
        a, b = lax.axis_index("gx"), lax.axis_index("gy")
        self.n_gy = len(peers_y) + 1
        self.total, self.g16, self.got_x, self.got_y, self.mine = total, g16, got_x, got_y, mine
        self.first = [remote(g16.at[p[0]], got_x.at[r], xs.at[r], xr.at[r], p) for r, p in enumerate(peers_x)]
        self.second = [
            remote(got_y.at[0], got_y.at[r + 1], ys.at[r], yr.at[r], p) for r, p in enumerate(peers_y)
        ]
        self.third = [remote(mine, total.at[a], zs.at[r], zr.at[r], p) for r, p in enumerate(peers_x)]

    def load(self, parts):
        flat = jnp.concatenate(parts, axis=0).astype(BF16)
        share = self.g16.shape[1]
        for i in range(self.g16.shape[0]):
            self.g16[i] = flat[i * share : (i + 1) * share]
        for copy in self.first:
            copy.start()

    def across(self):
        acc = self.g16[lax.axis_index("gx")].astype(F32)
        for r, copy in enumerate(self.first):
            copy.wait_recv()
            acc = acc + self.got_x[r].astype(F32)
        self.got_y[0] = acc.astype(BF16)
        for copy in self.second:
            copy.start()

    def along(self):
        a, b = lax.axis_index("gx"), lax.axis_index("gy")
        for copy in self.second:
            copy.wait_recv()
        acc = jnp.zeros(self.mine.shape, F32)
        for y in range(self.n_gy):
            acc = acc + self.got_y[lax.rem(b - y + self.n_gy, self.n_gy)].astype(F32)
        self.mine[...] = acc.astype(BF16)
        for copy in self.third:
            copy.start()
        self.total[a] = acc.astype(BF16)

    def finish(self):
        for copy in self.third:
            copy.wait_recv()
        for copy in self.first + self.second + self.third:
            copy.wait_send()


def main_kernel(
    n_gx, n_gy, chunk,
    ecount_in, nodes_in, rows_in, gcount_in, send_in, recv_in, pool_in,
    wei_in, weo_in, wni_in, wno_in, wci_in, wco_in, d_fine_in, d_coarse_in,
    fine_ref, coarse_ref, grad_ref, early_ref, late_ref,
    ecount_ref, nodes_ref, rows_ref, gcount_ref, send_ref, recv_ref, pool_ref,
    wei_ref, weo_ref, wni_ref, wno_ref, wci_ref, wco_ref, d_fine_ref, d_coarse_ref, load_sem,
    outgoing, arrived, back_out, back, nodes_wide, ghost_wide, ghost_fold,
    srow, rrow, s_fold, r_fold, s_fold16, r_fold16, s_lanes, r_lanes,
    pairs, edge16, slope_ref, wide_r, wide_s, both, agg, node_slope, d_node_ref,
    rims, got_rims, got_dc, g_in,
    e16, e_x, e_y, e_mine, l16, l_x, l_y, l_mine,
    out_s, out_r, ret_s, ret_r, rim_s, rim_r,
    exs, exr, eys, eyr, ezs, ezr, lxs, lxr, lys, lyr, lzs, lzr,
):
    rows, latent = nodes_ref.shape
    edges_n = send_ref.shape[1]
    peers, slots = rows_ref.shape[1:]
    co = d_coarse_ref.shape[0]
    bits = slots.bit_length() - 1
    own = rows // slots
    a, b = lax.axis_index("gx"), lax.axis_index("gy")
    found = neighbours(n_gx, n_gy, 1)
    returns = neighbours(n_gx, n_gy, -1)
    peers_x = [(lax.rem(a + r, n_gx), b) for r in range(1, n_gx)]
    peers_y = [(a, lax.rem(b + r, n_gy)) for r in range(1, n_gy)]
    corners = [f for f, dx, dy in zip(found, ACROSS, ALONG) if dx and dy]

    loads = [
        pltpu.make_async_copy(src, dst, load_sem.at[i])
        for i, (src, dst) in enumerate((
            (rows_in, rows_ref), (gcount_in, gcount_ref), (nodes_in, nodes_ref), (d_coarse_in, d_coarse_ref),
            (send_in, send_ref), (recv_in, recv_ref), (ecount_in, ecount_ref), (wei_in, wei_ref), (weo_in, weo_ref), (wni_in, wni_ref),
            (wno_in, wno_ref), (pool_in, pool_ref), (wco_in, wco_ref), (wci_in, wci_ref), (d_fine_in, d_fine_ref)))
    ]
    for load in loads:
        load.start()
    barrier = pltpu.get_barrier_semaphore()
    expect = jnp.int32(n_gx + n_gy - 2)
    for target, there, _ in corners:
        @pl.when(there)
        def _(target=target):
            pl.semaphore_signal(barrier, inc=1, device_id=target, device_id_type=MESH)
        expect = expect + jnp.where(there, 1, 0)
    for peer in peers_x + peers_y:
        pl.semaphore_signal(barrier, inc=1, device_id=peer, device_id_type=MESH)

    sent = exchange_copies(found, outgoing, arrived, out_s, out_r)
    returned = exchange_copies(returns, back_out, back, ret_s, ret_r)
    dc_rims = Rims(n_gy, d_coarse_ref.at[:BAND], d_coarse_ref.at[co - BAND :], got_dc, rim_s.at[0], rim_r.at[0])
    pool_rims = Rims(n_gy, rims.at[0], rims.at[1], got_rims, rim_s.at[1], rim_r.at[1])
    early = Total(peers_x, peers_y, early_ref, e16, e_x, e_y, e_mine, exs, exr, eys, eyr, ezs, ezr)
    late = Total(peers_x, peers_y, late_ref, l16, l_x, l_y, l_mine, lxs, lxr, lys, lyr, lzs, lzr)

    def code(index):
        fold = (index >> bits) & (FOLDS - 1)
        group = jnp.where(index < 0, NOWHERE, (index >> bits) // FOLDS * slots + (index & (slots - 1)))
        return (fold << 16) | group

    def decode(row):
        col = columns(row)
        fold = col >> 16
        return col.astype(jnp.int16), fold, fold.astype(jnp.int16)

    def place(index, group):
        mine = (index >= group * FOLDS * slots) & (index < (group + 1) * FOLDS * slots)
        return jnp.where(mine, index & (slots - 1), -1)

    def ghost_row(k):
        return alive(rows_ref[0, k : k + 1, :], 0, gcount_ref[:, k : k + 1])

    for load in loads[:3]:
        load.wait()
    for j in range(own):
        nodes_wide[:, j * latent : (j + 1) * latent] = nodes_ref[j * slots : (j + 1) * slots]
    for at in range(0, peers, FOLDS):
        batch = SEND_ORDER[at : at + FOLDS]
        where, fold, fold16 = decode(jnp.concatenate([code(ghost_row(k)) for k in batch], axis=1))
        picked = choose(fold, mm(pick_lanes(where, 0, slots), nodes_wide[...])).astype(BF16)
        for n, k in enumerate(batch):
            ghost_fold[k] = fold16[n * slots : (n + 1) * slots]
            outgoing[k] = picked[n * slots : (n + 1) * slots]
        if at == 0:
            pl.semaphore_wait(barrier, expect)
        for k in batch:
            start(found, sent, k)
    for load in loads[3:]:
        load.wait()
    dc_rims.start()
    clear_absent(found, arrived)
    clear_absent(returns, back)

    send = send_ref[...]
    moved = send
    for p, k in enumerate(GHOST_ORDER):
        moved = jnp.where((send >> bits) == own + k, (send & (slots - 1)) + ((own + p) << bits), moved)
    srow[...] = moved
    rrow[...] = alive(recv_ref[...], 0, ecount_ref[0])

    def first_pass(i, carry):
        at = pl.ds(pl.multiple_of(i * chunk, chunk), chunk)
        s_where, s_f, s_fold16[at, :] = decode(code(srow[:, at]))
        r_where, r_f, r_fold16[at, :] = decode(code(rrow[:, at]))
        s_fold[at, :] = s_f
        r_fold[at, :] = r_f
        for t in range(s_lanes.shape[0]):
            s_lanes[t, at, :] = pick_lanes(s_where, t * slots, slots)
        r_lanes[at, :] = pick_lanes(r_where, 0, slots)
        pairs[at, :latent] = choose(s_f, mm(s_lanes[0, at, :], nodes_wide[...])).astype(BF16)
        pairs[at, latent:] = choose(r_f, mm(r_lanes[at, :], nodes_wide[...])).astype(BF16)
        return carry

    steps = edges_n // chunk
    lax.fori_loop(0, steps, first_pass, 0)

    def take_ghosts(group):
        for j, k in enumerate(GHOST_ORDER[group * FOLDS : (group + 1) * FOLDS]):
            wait_recv(found, sent, k)
        for j, k in enumerate(GHOST_ORDER[group * FOLDS : (group + 1) * FOLDS]):
            ghost_wide[:, j * latent : (j + 1) * latent] = arrived[k]

    take_ghosts(0)

    def second_pass(i, carry):
        at = pl.ds(pl.multiple_of(i * chunk, chunk), chunk)
        got = choose(s_fold[at, :], mm(s_lanes[1, at, :], ghost_wide[...])).astype(BF16)
        pairs[at, :latent] = pairs[at, :latent] + got
        return carry

    lax.fori_loop(0, steps, second_pass, 0)
    take_ghosts(1)

    def third_pass(i, carry):
        at = pl.ds(pl.multiple_of(i * chunk, chunk), chunk)
        got = choose(s_fold[at, :], mm(s_lanes[2, at, :], ghost_wide[...])).astype(BF16)
        pairs[at, :latent] = pairs[at, :latent] + got
        pre = mm(pairs[at, :], wei_ref[...])
        s = sigmoid(pre)
        act = pre * s
        slope_ref[at, :] = s + act * (1.0 - s)
        wide_r[at, :] = spread(act.astype(BF16), r_fold16[at, :])
        return carry

    lax.fori_loop(0, steps, third_pass, 0)

    both[:, :latent] = nodes_ref[...]
    acts = mm(pick_sublanes(place(rrow[...], 0), slots), wide_r[...]).astype(BF16)
    for j in range(FOLDS):
        agg[j * slots : (j + 1) * slots, :] = piece(acts, j)
    both[:, latent:] = mm(agg[...], weo_ref[...]).astype(BF16)
    node_pre = mm(both[...], wni_ref[...])
    s = sigmoid(node_pre)
    node_act = (node_pre * s).astype(BF16)
    node_slope[...] = slope(s, node_pre)
    fine = (nodes_ref[...].astype(F32) + mm(node_act, wno_ref[...])).astype(BF16)
    fine_ref[...] = fine
    window = mm(pick_sublanes(pool_ref[...], co + 2 * BAND), fine)
    rims[0] = window[: 2 * BAND].astype(BF16)
    rims[1] = window[co:].astype(BF16)
    pool_rims.start()

    dc_rims.wait()
    d_coarse = d_coarse_ref[...]
    d_wide = jnp.concatenate([got_dc[0], d_coarse, got_dc[1]], axis=0)
    d_act = mm_t(d_wide, wco_ref[...])
    pool_hot = pick_lanes(columns(pool_ref[...]).astype(jnp.int16), 0, co + 2 * BAND)
    pool_rims.wait()
    coarse_in = (0.125 * jnp.concatenate(
        [
            window[: 2 * BAND] + got_rims[0].astype(F32),
            window[2 * BAND : co],
            window[co:] + got_rims[1].astype(F32),
        ],
        axis=0,
    )).astype(BF16)
    pre = mm(coarse_in, wci_ref[...])
    s = sigmoid(pre)
    d_pre = (d_act * slope(s, pre)).astype(BF16)
    reach = (d_wide.astype(F32) + mm_t(d_pre, wci_ref[...])).astype(BF16)

    d_total = d_fine_ref[...].astype(F32) + 0.125 * mm(pool_hot, reach)
    d16 = d_total.astype(BF16)
    d_node = (mm_t(d16, wno_ref[...]) * node_slope[...]).astype(BF16)
    d_summed = mm_t(d_node, wni_ref[latent:, :]).astype(BF16)
    d_edge_out = mm_t(d_summed, weo_ref[...]).astype(BF16)
    for j in range(FOLDS):
        ghost_wide[:, j * latent : (j + 1) * latent] = d_edge_out[j * slots : (j + 1) * slots]
    d_node_ref[...] = d_node
    grad_ref[...] = d_total
    mid = slice(BAND, co + BAND)
    act = (pre * s)[mid].astype(BF16)
    coarse_ref[...] = (coarse_in[mid].astype(F32) + mm(act, wco_ref[...])).astype(BF16)
    early.load([
        t_mm(both[...], d_node), t_mm(node_act, d16), t_mm(coarse_in[mid], d_pre[mid]), t_mm(act, d_coarse),
        t_mm(agg[...], d_summed)])
    g_in[...] = jnp.zeros_like(g_in)

    def back_pass(i, carry):
        at = pl.ds(pl.multiple_of(i * chunk, chunk), chunk)
        d_act = choose(r_fold[at, :], mm(r_lanes[at, :], ghost_wide[...]))
        d_edge = (d_act * slope_ref[at, :]).astype(BF16)
        edge16[at, :] = d_edge
        g_in[...] += t_mm(pairs[at, :], d_edge)
        return carry

    lax.fori_loop(0, steps, back_pass, 0)
    late.load([g_in[...]])
    w_send, w_recv = wei_ref[:latent, :], wei_ref[latent:, :]

    def send_sums(group):
        return mm(pick_sublanes(place(srow[...], group), slots), wide_s[...]).astype(BF16)

    def ghost_sums(group):
        sums = send_sums(1 + group)
        for j, k in enumerate(GHOST_ORDER[group * FOLDS : (group + 1) * FOLDS]):
            back_out[k] = mm_t(piece(sums, j), w_send).astype(BF16)

    def give_back(group):
        for k in GHOST_ORDER[group * FOLDS : (group + 1) * FOLDS]:
            start(returns, returned, k)

    def add_sums(sums, w):
        for j in range(FOLDS):
            grad_ref[j * slots : (j + 1) * slots, :] += mm_t(piece(sums, j), w)

    def receiver_sums():
        wide_r[...] = spread(edge16[...], r_fold16[...])
        add_sums(mm(pick_sublanes(place(rrow[...], 0), slots), wide_r[...]).astype(BF16), w_recv)

    def own_sums():
        add_sums(send_sums(0), w_send)
        grad_ref[...] += mm_t(d_node_ref[...], wni_ref[:latent, :])

    def add_returns(group):
        ks = GHOST_ORDER[group * FOLDS : (group + 1) * FOLDS]
        for n, k in enumerate(ks):
            wait_recv(returns, returned, k)
            wide_r[n * slots : (n + 1) * slots, :] = spread(back[k], ghost_fold[k])
        ghosts = jnp.concatenate([place(ghost_row(k), 0) for k in ks], axis=1)
        sums = mm(pick_sublanes(ghosts, slots), wide_r[: FOLDS * slots, :])
        for j in range(FOLDS):
            grad_ref[j * slots : (j + 1) * slots, :] += piece(sums, j)

    wide_s[...] = spread(edge16[...], s_fold16[...])
    ghost_sums(0)
    give_back(0)
    receiver_sums()
    early.across()
    own_sums()
    late.across()
    ghost_sums(1)
    early.along()
    give_back(1)
    add_returns(0)
    late.along()
    add_returns(1)
    early.finish()
    late.finish()
    wait_sends(found, sent)
    wait_sends(returns, returned)
    dc_rims.drain()
    pool_rims.drain()


def final_kernel(
    scale, fine_in, coarse_in, grad_in, early_in, late_in,
    fine_out, coarse_out, grad_out, ei_ref, eo_ref, ni_ref, no_ref, ci_ref, co_ref,
):
    fine_out[...] = fine_in[...]
    coarse_out[...] = coarse_in[...]
    grad_out[...] = grad_in[...]

    def put(total_ref, refs):
        flat = total_ref[...].reshape(-1, total_ref.shape[-1]).astype(F32) * scale
        at = 0
        for ref in refs:
            ref[...] = flat[at : at + ref.shape[0]]
            at += ref.shape[0]

    put(early_in, (ni_ref, no_ref, ci_ref, co_ref, eo_ref))
    put(late_in, (ei_ref,))


def body(
    n_gx, n_gy, nodes, ghost_rows, ghost_count, edge_send, edge_recv, edge_count, pool_map,
    w_edge_in, w_edge_out, w_node_in, w_node_out, w_coarse_in, w_coarse_out, d_fine, d_coarse,
):
    rows, latent = nodes.shape
    _, peers, slots = ghost_rows.shape
    edges_n = edge_send.shape[1]
    co = d_coarse.shape[0]
    chunk = edges_n
    groups = (rows // slots + peers) // FOLDS
    dma = pltpu.SemaphoreType.DMA
    vmem = pl.BlockSpec(memory_space=pltpu.VMEM)
    hbm = pl.BlockSpec(memory_space=pltpu.HBM)
    early_rows, late_rows = 6 * latent // n_gx, 2 * latent // n_gx

    def total_buffers(share):
        return [
            pltpu.VMEM((n_gx, share, latent), BF16), pltpu.VMEM((n_gx - 1, share, latent), BF16),
            pltpu.VMEM((n_gy, share, latent), BF16), pltpu.VMEM((share, latent), BF16)]

    total_sems = [dma((n_gx - 1,))] * 2 + [dma((n_gy - 1,))] * 2 + [dma((n_gx - 1,))] * 2
    halo = pltpu.VMEM((peers, slots, latent), BF16)
    arrays = (edge_count, nodes, ghost_rows, ghost_count, edge_send, edge_recv, pool_map, w_edge_in, w_edge_out,
              w_node_in, w_node_out, w_coarse_in, w_coarse_out, d_fine, d_coarse)
    results = pl.pallas_call(
        functools.partial(main_kernel, n_gx, n_gy, chunk),
        out_shape=[
            jax.ShapeDtypeStruct((rows, latent), BF16), jax.ShapeDtypeStruct((co, latent), BF16),
            jax.ShapeDtypeStruct((rows, latent), F32),
            jax.ShapeDtypeStruct((n_gx, early_rows, latent), BF16),
            jax.ShapeDtypeStruct((n_gx, late_rows, latent), BF16)],
        in_specs=[pl.BlockSpec(memory_space=pl.ANY)] + [hbm] * (len(arrays) - 1),
        out_specs=[vmem] * 5,
        scratch_shapes=[pltpu.SMEM((1,), jnp.int32)] + [pltpu.VMEM(x.shape, x.dtype) for x in arrays[1:]] + [dma((len(arrays),))] + [halo] * 4 + [
            pltpu.VMEM((slots, FOLDS * latent), BF16), pltpu.VMEM((slots, FOLDS * latent), BF16),
            pltpu.VMEM((peers, slots, LANES), jnp.int16),
            pltpu.VMEM((1, edges_n), jnp.int32), pltpu.VMEM((1, edges_n), jnp.int32),
            pltpu.VMEM((edges_n, LANES), jnp.int32), pltpu.VMEM((edges_n, LANES), jnp.int32),
            pltpu.VMEM((edges_n, LANES), jnp.int16), pltpu.VMEM((edges_n, LANES), jnp.int16),
            pltpu.VMEM((groups, edges_n, slots), BF16), pltpu.VMEM((edges_n, slots), BF16),
            pltpu.VMEM((edges_n, 2 * latent), BF16), pltpu.VMEM((edges_n, latent), BF16),
            pltpu.VMEM((edges_n, latent), F32),
            pltpu.VMEM((edges_n, FOLDS * latent), BF16), pltpu.VMEM((edges_n, FOLDS * latent), BF16),
            pltpu.VMEM((rows, 2 * latent), BF16), pltpu.VMEM((rows, latent), BF16),
            pltpu.VMEM((rows, latent), F32), pltpu.VMEM((rows, latent), BF16),
            pltpu.VMEM((2, 2 * BAND, latent), BF16), pltpu.VMEM((2, 2 * BAND, latent), BF16),
            pltpu.VMEM((2, BAND, latent), BF16),
            pltpu.VMEM((2 * latent, latent), F32),
        ] + total_buffers(early_rows) + total_buffers(late_rows)
        + [dma((peers,))] * 4 + [dma((2, 2))] * 2 + total_sems * 2,
        compiler_params=pltpu.CompilerParams(
            vmem_limit_bytes=48 * 1024 * 1024, collective_id=0, has_side_effects=True),
    )(edge_count, *(pltpu.with_memory_space_constraint(x, pltpu.HBM) for x in arrays[1:]))
    scale = 1.0 / (rows * n_gx * n_gy) ** 0.5
    fine, coarse, grads, ei, eo, ni, no, ci, co_grad = pl.pallas_call(
        functools.partial(final_kernel, scale),
        out_shape=[
            jax.ShapeDtypeStruct((rows, latent), BF16), jax.ShapeDtypeStruct((co, latent), BF16),
            jax.ShapeDtypeStruct((rows, latent), F32)] + [
            jax.ShapeDtypeStruct((n * latent, latent), F32) for n in (2, 1, 2, 1, 1, 1)],
        in_specs=[vmem] * 5,
        out_specs=[vmem] * 9,
        compiler_params=pltpu.CompilerParams(vmem_limit_bytes=8 * 1024 * 1024),
    )(*results)
    return fine, coarse, grads, ei, eo, ni, no, ci, co_grad


def solution(mesh):
    split = P(("gx", "gy"), None)
    return jax.shard_map(
        functools.partial(body, mesh.shape["gx"], mesh.shape["gy"]),
        mesh=mesh,
        in_specs=(split, P(("gx", "gy"), None, None), split, split, split, P(("gx", "gy")), split)
        + (P(),) * 6
        + (split, split),
        out_specs=(split, split, split) + (P(),) * 6,
        check_vma=False,
    )
```

```python
import functools

import jax
import jax.numpy as jnp
from jax import lax
from jax.experimental import pallas as pl
from jax.experimental.pallas import tpu as pltpu
from jax.sharding import PartitionSpec as P

BAND = 32
MESH = pl.DeviceIdType.MESH
ACROSS = (-1, -1, -1, 0, 0, 1, 1, 1)
ALONG = (-1, 0, 1, -1, 1, -1, 0, 1)
SEND_ORDER = (3, 4, 1, 6, 0, 2, 5, 7)
GHOST_ORDER = (1, 6, 3, 4, 0, 2, 5, 7)
F32 = jnp.float32
BF16 = jnp.bfloat16
FOLDS = 4
NOWHERE = 32767
LANES = 128


def mm(a, b):
    return jnp.dot(a, b, preferred_element_type=F32)


def mm_t(a, b):
    return lax.dot_general(a, b, (((1,), (1,)), ((), ())), preferred_element_type=F32)


def t_mm(a, b):
    return lax.dot_general(a, b, (((0,), (0,)), ((), ())), preferred_element_type=F32)


def sigmoid(v):
    return 0.5 * jnp.tanh(0.5 * v) + 0.5


def columns(row):
    return jnp.concatenate(
        [
            jnp.transpose(jnp.broadcast_to(row[:, s : s + LANES], (LANES, LANES)))
            for s in range(0, row.shape[1], LANES)
        ],
        axis=0,
    )


def alive(row, start, count):
    ids = lax.broadcasted_iota(jnp.int32, row.shape, 1) + start
    return jnp.where(ids < count, row, -1)


def hot(ids, index):
    return jnp.where(ids == index, jnp.ones((), BF16), jnp.zeros((), BF16))


def pick_lanes(col, first, width):
    ids = lax.broadcasted_iota(jnp.int16, (col.shape[0], LANES), 1)
    parts = [
        hot(ids + jnp.int16(first + s), col)[:, : min(LANES, width - s)] for s in range(0, width, LANES)
    ]
    return jnp.concatenate(parts, axis=1)


def pick_sublanes(row, height):
    return hot(lax.broadcasted_iota(jnp.int16, (height, row.shape[1]), 0), row.astype(jnp.int16))


def choose(fold, wide):
    width = wide.shape[1] // FOLDS
    out = wide[:, :width]
    for j in range(1, FOLDS):
        out = jnp.where(fold == j, wide[:, j * width : (j + 1) * width], out)
    return out


def spread(values, fold):
    return jnp.concatenate(
        [jnp.where(fold == jnp.int16(j), values, jnp.zeros((), BF16)) for j in range(FOLDS)], axis=1
    )


def piece(sums, j):
    width = sums.shape[1] // FOLDS
    return sums[:, j * width : (j + 1) * width]


def slope(s, v):
    return s * (1.0 + v * (1.0 - s))


def neighbours(n_gx, n_gy, sign):
    a, b = lax.axis_index("gx"), lax.axis_index("gy")
    found = []
    for dx, dy in zip(ACROSS, ALONG):
        dx, dy = sign * dx, sign * dy
        ta, tb = a + dx, b + dy
        sa, sb = a - dx, b - dy
        there = (ta >= 0) & (ta < n_gx) & (tb >= 0) & (tb < n_gy)
        here = (sa >= 0) & (sa < n_gx) & (sb >= 0) & (sb < n_gy)
        target = (jnp.clip(ta, 0, n_gx - 1), jnp.clip(tb, 0, n_gy - 1))
        found.append((target, there, here))
    return found


def remote(src, dst, send, recv, peer):
    return pltpu.make_async_remote_copy(
        src_ref=src, dst_ref=dst, send_sem=send, recv_sem=recv, device_id=peer, device_id_type=MESH)


def exchange_copies(found, src_ref, dst_ref, send_sem, recv_sem):
    return [
        remote(src_ref.at[k], dst_ref.at[k], send_sem.at[k], recv_sem.at[k], found[k][0])
        for k in range(len(found))
    ]


def clear_absent(found, dst_ref):
    for k in range(len(found)):
        @pl.when(jnp.logical_not(found[k][2]))
        def _(k=k):
            dst_ref[k] = jnp.zeros(dst_ref.shape[1:], dst_ref.dtype)


def start(found, copies, k):
    @pl.when(found[k][1])
    def _():
        copies[k].start()


def wait_recv(found, copies, k):
    @pl.when(found[k][2])
    def _():
        copies[k].wait_recv()


def wait_sends(found, copies):
    for k in range(len(found)):
        @pl.when(found[k][1])
        def _(k=k):
            copies[k].wait_send()


class Rims:
    def __init__(self, n_gy, low, high, got, send_sem, recv_sem):
        a, b = lax.axis_index("gx"), lax.axis_index("gy")
        self.below, self.above = b > 0, b < n_gy - 1
        self.down = remote(low, got.at[1], send_sem.at[0], recv_sem.at[1], (a, jnp.maximum(b - 1, 0)))
        self.up = remote(high, got.at[0], send_sem.at[1], recv_sem.at[0], (a, jnp.minimum(b + 1, n_gy - 1)))
        self.got = got

    def start(self):
        @pl.when(self.below)
        def _():
            self.down.start()

        @pl.when(self.above)
        def _():
            self.up.start()

        for slot, there in ((0, self.below), (1, self.above)):
            @pl.when(jnp.logical_not(there))
            def _(slot=slot):
                self.got[slot] = jnp.zeros(self.got.shape[1:], self.got.dtype)

    def wait(self):
        @pl.when(self.below)
        def _():
            self.up.wait_recv()

        @pl.when(self.above)
        def _():
            self.down.wait_recv()

    def drain(self):
        @pl.when(self.below)
        def _():
            self.down.wait_send()

        @pl.when(self.above)
        def _():
            self.up.wait_send()


class Total:
    def __init__(self, peers_x, peers_y, total, g16, got_x, got_y, mine, xs, xr, ys, yr, zs, zr):
        a, b = lax.axis_index("gx"), lax.axis_index("gy")
        self.n_gy = len(peers_y) + 1
        self.total, self.g16, self.got_x, self.got_y, self.mine = total, g16, got_x, got_y, mine
        self.first = [remote(g16.at[p[0]], got_x.at[r], xs.at[r], xr.at[r], p) for r, p in enumerate(peers_x)]
        self.second = [
            remote(got_y.at[0], got_y.at[r + 1], ys.at[r], yr.at[r], p) for r, p in enumerate(peers_y)
        ]
        self.third = [remote(mine, total.at[a], zs.at[r], zr.at[r], p) for r, p in enumerate(peers_x)]

    def load(self, parts):
        flat = jnp.concatenate(parts, axis=0).astype(BF16)
        share = self.g16.shape[1]
        for i in range(self.g16.shape[0]):
            self.g16[i] = flat[i * share : (i + 1) * share]
        for copy in self.first:
            copy.start()

    def across(self):
        acc = self.g16[lax.axis_index("gx")].astype(F32)
        for r, copy in enumerate(self.first):
            copy.wait_recv()
            acc = acc + self.got_x[r].astype(F32)
        self.got_y[0] = acc.astype(BF16)
        for copy in self.second:
            copy.start()

    def along(self):
        a, b = lax.axis_index("gx"), lax.axis_index("gy")
        for copy in self.second:
            copy.wait_recv()
        acc = jnp.zeros(self.mine.shape, F32)
        for y in range(self.n_gy):
            acc = acc + self.got_y[lax.rem(b - y + self.n_gy, self.n_gy)].astype(F32)
        self.mine[...] = acc.astype(BF16)
        for copy in self.third:
            copy.start()
        self.total[a] = acc.astype(BF16)

    def finish(self):
        for copy in self.third:
            copy.wait_recv()
        for copy in self.first + self.second + self.third:
            copy.wait_send()


def main_kernel(
    n_gx, n_gy, chunk,
    ecount_in, nodes_in, rows_in, gcount_in, send_in, recv_in, pool_in,
    wei_in, weo_in, wni_in, wno_in, wci_in, wco_in, d_fine_in, d_coarse_in,
    fine_ref, coarse_ref, grad_ref, early_ref, late_ref,
    ecount_ref, nodes_ref, rows_ref, gcount_ref, send_ref, recv_ref, pool_ref,
    wei_ref, weo_ref, wni_ref, wno_ref, wci_ref, wco_ref, d_fine_ref, d_coarse_ref, load_sem,
    outgoing, arrived, back_out, back, nodes_wide, ghost_wide, ghost_fold,
    srow, rrow, s_fold, r_fold, s_fold16, r_fold16, s_lanes, r_lanes,
    pairs, edge16, slope_ref, wide_r, wide_s, both, agg, node_slope, d_node_ref,
    rims, got_rims, got_dc, g_in,
    e16, e_x, e_y, e_mine, l16, l_x, l_y, l_mine,
    out_s, out_r, ret_s, ret_r, rim_s, rim_r,
    exs, exr, eys, eyr, ezs, ezr, lxs, lxr, lys, lyr, lzs, lzr,
):
    rows, latent = nodes_ref.shape
    edges_n = send_ref.shape[1]
    peers, slots = rows_ref.shape[1:]
    co = d_coarse_ref.shape[0]
    bits = slots.bit_length() - 1
    own = rows // slots
    a, b = lax.axis_index("gx"), lax.axis_index("gy")
    found = neighbours(n_gx, n_gy, 1)
    returns = neighbours(n_gx, n_gy, -1)
    peers_x = [(lax.rem(a + r, n_gx), b) for r in range(1, n_gx)]
    peers_y = [(a, lax.rem(b + r, n_gy)) for r in range(1, n_gy)]
    corners = [f for f, dx, dy in zip(found, ACROSS, ALONG) if dx and dy]

    loads = [
        pltpu.make_async_copy(src, dst, load_sem.at[i])
        for i, (src, dst) in enumerate((
            (rows_in, rows_ref), (gcount_in, gcount_ref), (nodes_in, nodes_ref), (d_coarse_in, d_coarse_ref),
            (send_in, send_ref), (recv_in, recv_ref), (ecount_in, ecount_ref), (wei_in, wei_ref), (weo_in, weo_ref), (wni_in, wni_ref),
            (wno_in, wno_ref), (pool_in, pool_ref), (wco_in, wco_ref), (wci_in, wci_ref), (d_fine_in, d_fine_ref)))
    ]
    for load in loads:
        load.start()
    barrier = pltpu.get_barrier_semaphore()
    expect = jnp.int32(n_gx + n_gy - 2)
    for target, there, _ in corners:
        @pl.when(there)
        def _(target=target):
            pl.semaphore_signal(barrier, inc=1, device_id=target, device_id_type=MESH)
        expect = expect + jnp.where(there, 1, 0)
    for peer in peers_x + peers_y:
        pl.semaphore_signal(barrier, inc=1, device_id=peer, device_id_type=MESH)

    sent = exchange_copies(found, outgoing, arrived, out_s, out_r)
    returned = exchange_copies(returns, back_out, back, ret_s, ret_r)
    dc_rims = Rims(n_gy, d_coarse_ref.at[:BAND], d_coarse_ref.at[co - BAND :], got_dc, rim_s.at[0], rim_r.at[0])
    pool_rims = Rims(n_gy, rims.at[0], rims.at[1], got_rims, rim_s.at[1], rim_r.at[1])
    early = Total(peers_x, peers_y, early_ref, e16, e_x, e_y, e_mine, exs, exr, eys, eyr, ezs, ezr)
    late = Total(peers_x, peers_y, late_ref, l16, l_x, l_y, l_mine, lxs, lxr, lys, lyr, lzs, lzr)

    def code(index):
        fold = (index >> bits) & (FOLDS - 1)
        group = jnp.where(index < 0, NOWHERE, (index >> bits) // FOLDS * slots + (index & (slots - 1)))
        return (fold << 16) | group

    def decode(row):
        col = columns(row)
        fold = col >> 16
        return col.astype(jnp.int16), fold, fold.astype(jnp.int16)

    def place(index, group):
        mine = (index >= group * FOLDS * slots) & (index < (group + 1) * FOLDS * slots)
        return jnp.where(mine, index & (slots - 1), -1)

    def ghost_row(k):
        return alive(rows_ref[0, k : k + 1, :], 0, gcount_ref[:, k : k + 1])

    for load in loads[:3]:
        load.wait()
    for j in range(own):
        nodes_wide[:, j * latent : (j + 1) * latent] = nodes_ref[j * slots : (j + 1) * slots]
    for at in range(0, peers, FOLDS):
        batch = SEND_ORDER[at : at + FOLDS]
        where, fold, fold16 = decode(jnp.concatenate([code(ghost_row(k)) for k in batch], axis=1))
        picked = choose(fold, mm(pick_lanes(where, 0, slots), nodes_wide[...])).astype(BF16)
        for n, k in enumerate(batch):
            ghost_fold[k] = fold16[n * slots : (n + 1) * slots]
            outgoing[k] = picked[n * slots : (n + 1) * slots]
        if at == 0:
            pl.semaphore_wait(barrier, expect)
        for k in batch:
            start(found, sent, k)
    for load in loads[3:]:
        load.wait()
    dc_rims.start()
    clear_absent(found, arrived)
    clear_absent(returns, back)

    send = send_ref[...]
    moved = send
    for p, k in enumerate(GHOST_ORDER):
        moved = jnp.where((send >> bits) == own + k, (send & (slots - 1)) + ((own + p) << bits), moved)
    srow[...] = moved
    rrow[...] = alive(recv_ref[...], 0, ecount_ref[0])

    def first_pass(i, carry):
        at = pl.ds(pl.multiple_of(i * chunk, chunk), chunk)
        s_where, s_f, s_fold16[at, :] = decode(code(srow[:, at]))
        r_where, r_f, r_fold16[at, :] = decode(code(rrow[:, at]))
        s_fold[at, :] = s_f
        r_fold[at, :] = r_f
        for t in range(s_lanes.shape[0]):
            s_lanes[t, at, :] = pick_lanes(s_where, t * slots, slots)
        r_lanes[at, :] = pick_lanes(r_where, 0, slots)
        pairs[at, :latent] = choose(s_f, mm(s_lanes[0, at, :], nodes_wide[...])).astype(BF16)
        pairs[at, latent:] = choose(r_f, mm(r_lanes[at, :], nodes_wide[...])).astype(BF16)
        return carry

    steps = edges_n // chunk
    lax.fori_loop(0, steps, first_pass, 0)

    def take_ghosts(group):
        for j, k in enumerate(GHOST_ORDER[group * FOLDS : (group + 1) * FOLDS]):
            wait_recv(found, sent, k)
        for j, k in enumerate(GHOST_ORDER[group * FOLDS : (group + 1) * FOLDS]):
            ghost_wide[:, j * latent : (j + 1) * latent] = arrived[k]

    take_ghosts(0)

    def second_pass(i, carry):
        at = pl.ds(pl.multiple_of(i * chunk, chunk), chunk)
        got = choose(s_fold[at, :], mm(s_lanes[1, at, :], ghost_wide[...])).astype(BF16)
        pairs[at, :latent] = pairs[at, :latent] + got
        return carry

    lax.fori_loop(0, steps, second_pass, 0)
    take_ghosts(1)

    def third_pass(i, carry):
        at = pl.ds(pl.multiple_of(i * chunk, chunk), chunk)
        got = choose(s_fold[at, :], mm(s_lanes[2, at, :], ghost_wide[...])).astype(BF16)
        pairs[at, :latent] = pairs[at, :latent] + got
        pre = mm(pairs[at, :], wei_ref[...])
        s = sigmoid(pre)
        act = pre * s
        slope_ref[at, :] = s + act * (1.0 - s)
        edge16[at, :] = act.astype(BF16)
        return carry

    lax.fori_loop(0, steps, third_pass, 0)

    both[:, :latent] = nodes_ref[...]
    acts = mm(pick_sublanes(place(rrow[...], 0), slots), spread(edge16[...], r_fold16[...])).astype(BF16)
    for j in range(FOLDS):
        agg[j * slots : (j + 1) * slots, :] = piece(acts, j)
    both[:, latent:] = mm(agg[...], weo_ref[...]).astype(BF16)
    node_pre = mm(both[...], wni_ref[...])
    s = sigmoid(node_pre)
    node_act = (node_pre * s).astype(BF16)
    node_slope[...] = slope(s, node_pre)
    fine = (nodes_ref[...].astype(F32) + mm(node_act, wno_ref[...])).astype(BF16)
    fine_ref[...] = fine
    window = mm(pick_sublanes(pool_ref[...], co + 2 * BAND), fine)
    rims[0] = window[: 2 * BAND].astype(BF16)
    rims[1] = window[co:].astype(BF16)
    pool_rims.start()

    dc_rims.wait()
    d_coarse = d_coarse_ref[...]
    d_wide = jnp.concatenate([got_dc[0], d_coarse, got_dc[1]], axis=0)
    d_act = mm_t(d_wide, wco_ref[...])
    pool_hot = pick_lanes(columns(pool_ref[...]).astype(jnp.int16), 0, co + 2 * BAND)
    pool_rims.wait()
    coarse_in = (0.125 * jnp.concatenate(
        [
            window[: 2 * BAND] + got_rims[0].astype(F32),
            window[2 * BAND : co],
            window[co:] + got_rims[1].astype(F32),
        ],
        axis=0,
    )).astype(BF16)
    pre = mm(coarse_in, wci_ref[...])
    s = sigmoid(pre)
    d_pre = (d_act * slope(s, pre)).astype(BF16)
    reach = (d_wide.astype(F32) + mm_t(d_pre, wci_ref[...])).astype(BF16)

    d_total = d_fine_ref[...].astype(F32) + 0.125 * mm(pool_hot, reach)
    d16 = d_total.astype(BF16)
    d_node = (mm_t(d16, wno_ref[...]) * node_slope[...]).astype(BF16)
    d_summed = mm_t(d_node, wni_ref[latent:, :]).astype(BF16)
    d_edge_out = mm_t(d_summed, weo_ref[...]).astype(BF16)
    for j in range(FOLDS):
        ghost_wide[:, j * latent : (j + 1) * latent] = d_edge_out[j * slots : (j + 1) * slots]
    d_node_ref[...] = d_node
    grad_ref[...] = d_total
    mid = slice(BAND, co + BAND)
    act = (pre * s)[mid].astype(BF16)
    coarse_ref[...] = (coarse_in[mid].astype(F32) + mm(act, wco_ref[...])).astype(BF16)
    early.load([
        t_mm(both[...], d_node), t_mm(node_act, d16), t_mm(coarse_in[mid], d_pre[mid]), t_mm(act, d_coarse),
        t_mm(agg[...], d_summed)])
    g_in[...] = jnp.zeros_like(g_in)

    def back_pass(i, carry):
        at = pl.ds(pl.multiple_of(i * chunk, chunk), chunk)
        d_act = choose(r_fold[at, :], mm(r_lanes[at, :], ghost_wide[...]))
        d_edge = (d_act * slope_ref[at, :]).astype(BF16)
        edge16[at, :] = d_edge
        g_in[...] += t_mm(pairs[at, :], d_edge)
        return carry

    lax.fori_loop(0, steps, back_pass, 0)
    late.load([g_in[...]])
    w_send, w_recv = wei_ref[:latent, :], wei_ref[latent:, :]

    def send_sums(group):
        return mm(pick_sublanes(place(srow[...], group), slots), wide_s[...]).astype(BF16)

    def ghost_sums(group):
        sums = send_sums(1 + group)
        for j, k in enumerate(GHOST_ORDER[group * FOLDS : (group + 1) * FOLDS]):
            back_out[k] = mm_t(piece(sums, j), w_send).astype(BF16)

    def give_back(group):
        for k in GHOST_ORDER[group * FOLDS : (group + 1) * FOLDS]:
            start(returns, returned, k)

    def add_sums(sums, w):
        for j in range(FOLDS):
            grad_ref[j * slots : (j + 1) * slots, :] += mm_t(piece(sums, j), w)

    def receiver_sums():
        hits = pick_sublanes(place(rrow[...], 0), slots)
        add_sums(mm(hits, spread(edge16[...], r_fold16[...])).astype(BF16), w_recv)

    def own_sums():
        add_sums(send_sums(0), w_send)
        grad_ref[...] += mm_t(d_node_ref[...], wni_ref[:latent, :])

    def add_returns(group):
        ks = GHOST_ORDER[group * FOLDS : (group + 1) * FOLDS]
        for n, k in enumerate(ks):
            wait_recv(returns, returned, k)
            wide_r[n * slots : (n + 1) * slots, :] = spread(back[k], ghost_fold[k])
        ghosts = jnp.concatenate([place(ghost_row(k), 0) for k in ks], axis=1)
        sums = mm(pick_sublanes(ghosts, slots), wide_r[: FOLDS * slots, :])
        for j in range(FOLDS):
            grad_ref[j * slots : (j + 1) * slots, :] += piece(sums, j)

    wide_s[...] = spread(edge16[...], s_fold16[...])
    ghost_sums(0)
    give_back(0)
    receiver_sums()
    early.across()
    own_sums()
    late.across()
    ghost_sums(1)
    early.along()
    give_back(1)
    add_returns(0)
    late.along()
    add_returns(1)
    early.finish()
    late.finish()
    wait_sends(found, sent)
    wait_sends(returns, returned)
    dc_rims.drain()
    pool_rims.drain()


def final_kernel(
    scale, fine_in, coarse_in, grad_in, early_in, late_in,
    fine_out, coarse_out, grad_out, ei_ref, eo_ref, ni_ref, no_ref, ci_ref, co_ref,
):
    fine_out[...] = fine_in[...]
    coarse_out[...] = coarse_in[...]
    grad_out[...] = grad_in[...]

    def put(total_ref, refs):
        flat = total_ref[...].reshape(-1, total_ref.shape[-1]).astype(F32) * scale
        at = 0
        for ref in refs:
            ref[...] = flat[at : at + ref.shape[0]]
            at += ref.shape[0]

    put(early_in, (ni_ref, no_ref, ci_ref, co_ref, eo_ref))
    put(late_in, (ei_ref,))


def body(
    n_gx, n_gy, nodes, ghost_rows, ghost_count, edge_send, edge_recv, edge_count, pool_map,
    w_edge_in, w_edge_out, w_node_in, w_node_out, w_coarse_in, w_coarse_out, d_fine, d_coarse,
):
    rows, latent = nodes.shape
    _, peers, slots = ghost_rows.shape
    edges_n = edge_send.shape[1]
    co = d_coarse.shape[0]
    chunk = edges_n
    groups = (rows // slots + peers) // FOLDS
    dma = pltpu.SemaphoreType.DMA
    vmem = pl.BlockSpec(memory_space=pltpu.VMEM)
    hbm = pl.BlockSpec(memory_space=pltpu.HBM)
    early_rows, late_rows = 6 * latent // n_gx, 2 * latent // n_gx

    def total_buffers(share):
        return [
            pltpu.VMEM((n_gx, share, latent), BF16), pltpu.VMEM((n_gx - 1, share, latent), BF16),
            pltpu.VMEM((n_gy, share, latent), BF16), pltpu.VMEM((share, latent), BF16)]

    total_sems = [dma((n_gx - 1,))] * 2 + [dma((n_gy - 1,))] * 2 + [dma((n_gx - 1,))] * 2
    halo = pltpu.VMEM((peers, slots, latent), BF16)
    arrays = (edge_count, nodes, ghost_rows, ghost_count, edge_send, edge_recv, pool_map, w_edge_in, w_edge_out,
              w_node_in, w_node_out, w_coarse_in, w_coarse_out, d_fine, d_coarse)
    results = pl.pallas_call(
        functools.partial(main_kernel, n_gx, n_gy, chunk),
        out_shape=[
            jax.ShapeDtypeStruct((rows, latent), BF16), jax.ShapeDtypeStruct((co, latent), BF16),
            jax.ShapeDtypeStruct((rows, latent), F32),
            jax.ShapeDtypeStruct((n_gx, early_rows, latent), BF16),
            jax.ShapeDtypeStruct((n_gx, late_rows, latent), BF16)],
        in_specs=[pl.BlockSpec(memory_space=pl.ANY)] + [hbm] * (len(arrays) - 1),
        out_specs=[vmem] * 5,
        scratch_shapes=[pltpu.SMEM((1,), jnp.int32)] + [pltpu.VMEM(x.shape, x.dtype) for x in arrays[1:]] + [dma((len(arrays),))] + [halo] * 4 + [
            pltpu.VMEM((slots, FOLDS * latent), BF16), pltpu.VMEM((slots, FOLDS * latent), BF16),
            pltpu.VMEM((peers, slots, LANES), jnp.int16),
            pltpu.VMEM((1, edges_n), jnp.int32), pltpu.VMEM((1, edges_n), jnp.int32),
            pltpu.VMEM((edges_n, LANES), jnp.int32), pltpu.VMEM((edges_n, LANES), jnp.int32),
            pltpu.VMEM((edges_n, LANES), jnp.int16), pltpu.VMEM((edges_n, LANES), jnp.int16),
            pltpu.VMEM((groups, edges_n, slots), BF16), pltpu.VMEM((edges_n, slots), BF16),
            pltpu.VMEM((edges_n, 2 * latent), BF16), pltpu.VMEM((edges_n, latent), BF16),
            pltpu.VMEM((edges_n, latent), F32),
            pltpu.VMEM((edges_n, FOLDS * latent), BF16), pltpu.VMEM((edges_n, FOLDS * latent), BF16),
            pltpu.VMEM((rows, 2 * latent), BF16), pltpu.VMEM((rows, latent), BF16),
            pltpu.VMEM((rows, latent), F32), pltpu.VMEM((rows, latent), BF16),
            pltpu.VMEM((2, 2 * BAND, latent), BF16), pltpu.VMEM((2, 2 * BAND, latent), BF16),
            pltpu.VMEM((2, BAND, latent), BF16),
            pltpu.VMEM((2 * latent, latent), F32),
        ] + total_buffers(early_rows) + total_buffers(late_rows)
        + [dma((peers,))] * 4 + [dma((2, 2))] * 2 + total_sems * 2,
        compiler_params=pltpu.CompilerParams(
            vmem_limit_bytes=48 * 1024 * 1024, collective_id=0, has_side_effects=True),
    )(edge_count, *(pltpu.with_memory_space_constraint(x, pltpu.HBM) for x in arrays[1:]))
    scale = 1.0 / (rows * n_gx * n_gy) ** 0.5
    fine, coarse, grads, ei, eo, ni, no, ci, co_grad = pl.pallas_call(
        functools.partial(final_kernel, scale),
        out_shape=[
            jax.ShapeDtypeStruct((rows, latent), BF16), jax.ShapeDtypeStruct((co, latent), BF16),
            jax.ShapeDtypeStruct((rows, latent), F32)] + [
            jax.ShapeDtypeStruct((n * latent, latent), F32) for n in (2, 1, 2, 1, 1, 1)],
        in_specs=[vmem] * 5,
        out_specs=[vmem] * 9,
        compiler_params=pltpu.CompilerParams(vmem_limit_bytes=8 * 1024 * 1024),
    )(*results)
    return fine, coarse, grads, ei, eo, ni, no, ci, co_grad


def solution(mesh):
    split = P(("gx", "gy"), None)
    return jax.shard_map(
        functools.partial(body, mesh.shape["gx"], mesh.shape["gy"]),
        mesh=mesh,
        in_specs=(split, P(("gx", "gy"), None, None), split, split, split, P(("gx", "gy")), split)
        + (P(),) * 6
        + (split, split),
        out_specs=(split, split, split) + (P(),) * 6,
        check_vma=False,
    )
```
